16 devices in a mesh: rep: 2 (over y, z), dp: 8 (over x, core).
Axes of the slice: x: 4, y: 2, z: 1, core: 2. Of those that a mesh axis runs over, the one named last changes fastest.
The devices are a block of a 4x4x8 slice.
Arguments:
- x: bfloat16 [16, 2048, 512], P(('rep', 'dp')), parts along dimension 0
- dy: bfloat16 [16, 2048, 512], P(('rep', 'dp')), parts along dimension 0
- w_gate: bfloat16 [2, 512, 2048], replicated
- w_up: bfloat16 [2, 512, 2048], replicated
- w_down: bfloat16 [2, 2048, 512], replicated
- m_w_gate: float32 [2, 512, 2048], replicated
- m_w_up: float32 [2, 512, 2048], replicated
- m_w_down: float32 [2, 2048, 512], replicated
- v_w_gate: float32 [2, 512, 2048], replicated
- v_w_up: float32 [2, 512, 2048], replicated
- v_w_down: float32 [2, 2048, 512], replicated
Outputs:
- output 1: bfloat16 [4, 512, 2048], P('rep'), parts along dimension 0
- output 2: bfloat16 [4, 512, 2048], P('rep'), parts along dimension 0
- output 3: bfloat16 [4, 2048, 512], P('rep'), parts along dimension 0
- output 4: float32 [4, 512, 2048], P('rep'), parts along dimension 0
- output 5: float32 [4, 512, 2048], P('rep'), parts along dimension 0
- output 6: float32 [4, 2048, 512], P('rep'), parts along dimension 0
- output 7: float32 [4, 512, 2048], P('rep'), parts along dimension 0
- output 8: float32 [4, 512, 2048], P('rep'), parts along dimension 0
- output 9: float32 [4, 2048, 512], P('rep'), parts along dimension 0
There are 2 independent parts. The reference program is written for one: setup_inputs(seed, part) draws one part's arguments, and reference() takes and returns one part's arrays. A program takes and returns all parts, laid end to end along the dimension named above; an argument that names none is the same for every part.
All inputs are finite; a program needn't handle non-finite values.
Results may differ from the reference program's by a relative error of at most 0.022.
Values are sent between devices in bfloat16 or wider.
A program may use at most 768 MiB of HBM per device.

```python
import jax
import jax.numpy as jnp
from jax import lax

SEQUENCES = 8
TOKENS = 2048
D = 512
FF = 2048
LAYERS = 2
NAMES = ("w_gate", "w_up", "w_down")
SHAPES = {"w_gate": (LAYERS, D, FF), "w_up": (LAYERS, D, FF), "w_down": (LAYERS, FF, D)}


def bump(key, n, height):
    away = (jnp.arange(n, dtype=jnp.int32) - jax.random.randint(key, (), 0, n, jnp.int32)) % n
    return jnp.where(away < n // 8, height, 1.0)


def together(key, own, strength):
    shared = jax.random.normal(key, own.shape[1:], jnp.float32)
    return (own + strength * shared) * lax.rsqrt(1 + strength * strength)


def setup_inputs(seed: int = 0, part: int = 0) -> dict:
    kx, kdy, ka, kb, kz, kf, kh, kl, *keys = jax.random.split(jax.random.key(seed), 8 + 3 * len(NAMES))
    kx, kdy, ka, kb = (jax.random.fold_in(k, part) for k in (kx, kdy, ka, kb))
    kw, km, kv = (keys[i::3] for i in range(3))
    shape = (SEQUENCES, TOKENS, D)
    much_x, much_dy = jax.random.uniform(kz, (2,), jnp.float32, 0.0, 1.0)
    loud = 2.0 ** jax.random.uniform(jax.random.fold_in(kz, 1), (), jnp.float32, -1.0, 2.0)
    layers = 2.0 ** jax.random.uniform(kl, (LAYERS, 1, 1), jnp.float32, -1.0, 1.0)
    x = together(ka, jax.random.normal(kx, shape, jnp.float32), much_x) * bump(kf, D, 4.0)
    dy = together(kb, jax.random.normal(kdy, shape, jnp.float32), much_dy)
    drawn = {"x": x.astype(jnp.bfloat16), "dy": (loud * dy * (SEQUENCES * TOKENS) ** -0.5).astype(jnp.bfloat16)}
    for key, name in zip(kw, NAMES, strict=True):
        w = jax.random.normal(key, SHAPES[name], jnp.float32) * SHAPES[name][1] ** -0.5
        drawn[name] = (w * {"w_gate": 1.0, "w_up": bump(kh, FF, 4.0), "w_down": layers}[name]).astype(jnp.bfloat16)
    for key, name in zip(km, NAMES, strict=True):
        drawn[f"m_{name}"] = 0.1 * jax.random.normal(key, SHAPES[name], jnp.float32)
    for key, name in zip(kv, NAMES, strict=True):
        drawn[f"v_{name}"] = jax.random.uniform(key, SHAPES[name], jnp.float32, 0.005, 0.015)
    return drawn


def matmul(a, w):
    return jnp.dot(a, w, preferred_element_type=jnp.float32).astype(jnp.bfloat16)


def normed(h):
    wide = h.astype(jnp.float32)
    scale = lax.rsqrt(jnp.mean(wide**2, -1, keepdims=True) + 1e-6)
    return (wide * scale).astype(jnp.bfloat16)


def layer(h, w):
    a = normed(h)
    gate = jnp.dot(a, w["w_gate"], preferred_element_type=jnp.float32)
    up = jnp.dot(a, w["w_up"], preferred_element_type=jnp.float32)
    return h + matmul((jax.nn.silu(gate) * up).astype(jnp.bfloat16), w["w_down"])


def adamw(w, m, v, g):
    m = 0.9 * m + 0.1 * g
    v = 0.95 * v + 0.05 * g * g
    step = m * lax.rsqrt(v + 1e-8) + 0.1 * w
    return (w - 0.02 * step).astype(jnp.bfloat16), m, v


def clipped(gradients, sum_of_squares, count):
    factor = jnp.minimum(1.0, 0.5 * lax.rsqrt(sum_of_squares / count + 1e-30))
    return [g * factor for g in gradients]


def stack(weights, h):
    return lax.scan(lambda h, w: (layer(h, w), None), h, weights)[0]


def reference(x, dy, w_gate, w_up, w_down, m_w_gate, m_w_up, m_w_down, v_w_gate, v_w_up, v_w_down):
    weights = dict(zip(NAMES, (w_gate, w_up, w_down), strict=True))

    def take(so_far, sequence):
        h, by_y = sequence
        _, back = jax.vjp(lambda w: stack(w, h), weights)
        return jax.tree.map(lambda total, term: total + term.astype(jnp.float32), so_far, back(by_y)[0]), None

    none_yet = {name: jnp.zeros(w.shape, jnp.float32) for name, w in weights.items()}
    by_weights, _ = lax.scan(take, none_yet, (x, dy))
    gradients = [by_weights[name].astype(jnp.bfloat16).astype(jnp.float32) for name in NAMES]
    gradients = clipped(gradients, sum(jnp.sum(g * g) for g in gradients), sum(g.size for g in gradients))
    new = [
        adamw(w.astype(jnp.float32), m, v, g)
        for w, m, v, g in zip((w_gate, w_up, w_down), (m_w_gate, m_w_up, m_w_down), (v_w_gate, v_w_up, v_w_down), gradients, strict=True)
    ]
    return tuple(one[which] for which in range(3) for one in new)
```

```python
import functools

import jax
import jax.numpy as jnp
from jax import lax
from jax.experimental import pallas as pl
from jax.experimental.pallas import tpu as pltpu
from jax.sharding import PartitionSpec as P

MESH = pl.DeviceIdType.MESH
BF16, F32 = jnp.bfloat16, jnp.float32
CORES = 2
CHUNK = 256
TILE = 512
FTILE = 256
SLOTS = 4
TERMS = 5
HALVES = 7
RUNS = 6
COMM = True


def dot(a, b):
    return jnp.dot(a, b, preferred_element_type=F32)


def dot_t(a, b):
    return lax.dot_general(a, b, (((1,), (1,)), ((), ())), preferred_element_type=F32)


def sigmoid(z):
    return 0.5 * jnp.tanh(0.5 * z) + 0.5


def norm_scale(wide):
    return lax.rsqrt(jnp.mean(wide * wide, -1, keepdims=True) + 1e-6)


def grad_kernel(
    dp, layers, x_hbm, dy_hbm, wg_hbm, wu_hbm, wd_hbm, g_hbm, ssq_out,
    xv, dyv, hv, av, at, dt, acc, actf, act, dgu, wgu, wd, term, from_core, run, g, ssq, ssq_all,
    io_sem, w_sem, out_sem, core_sem, ring_send, ring_recv, near_send, near_recv, far_send, far_recv, half_sem, ssq_send, ssq_recv,
):
    tokens, d = xv.shape
    ff = wd_hbm.shape[1]
    per = ff // CHUNK
    total = layers * per
    chips = dp // CORES
    rows = g.shape[1]
    half = rows // CORES
    own = half // chips
    piece = own // 2
    rep = lax.axis_index("rep")
    me = lax.axis_index("dp")
    chip, core = me // CORES, me % CORES
    other = 1 - core

    def device(chip, core):
        return (rep, chip * CORES + core)

    right, left = device((chip + 1) % chips, core), device((chip + chips - 1) % chips, core)
    sibling = device(chip, other)

    barrier = pltpu.get_barrier_semaphore()
    if COMM:
        for k in range(1, dp):
            pl.semaphore_signal(barrier, inc=1, device_id=(rep, (me + k) % dp), device_id_type=MESH)

    def load_x():
        return pltpu.make_async_copy(x_hbm, xv, io_sem.at[0])

    def load_dy():
        return pltpu.make_async_copy(dy_hbm, dyv, io_sem.at[1])

    def load_w(layer):
        copies = []
        for c in range(per):
            cut = slice(c * CHUNK, (c + 1) * CHUNK)
            copies.append(pltpu.make_async_copy(wg_hbm.at[layer, :, cut], wgu.at[layer, c, :, :CHUNK], w_sem.at[layer, c, 0]))
            copies.append(pltpu.make_async_copy(wu_hbm.at[layer, :, cut], wgu.at[layer, c, :, CHUNK:], w_sem.at[layer, c, 1]))
            copies.append(pltpu.make_async_copy(wd_hbm.at[layer, cut, :], wd.at[layer, cut, :], w_sem.at[layer, c, 2]))
        return copies

    load_x().start()
    for copy in load_w(0):
        copy.start()
    load_dy().start()
    for copy in load_w(1):
        copy.start()

    load_x().wait()
    for copy in load_w(0):
        copy.wait()
    load_dy().wait()

    @pl.loop(0, tokens // FTILE)
    def _(t):
        at_t = pl.ds(pl.multiple_of(t * FTILE, FTILE), FTILE)
        wide = xv[at_t, :].astype(F32)
        a = (wide * norm_scale(wide)).astype(BF16)
        for c in range(per):
            gu = dot(a, wgu[0, c])
            gate, up = gu[:, :CHUNK], gu[:, CHUNK:]
            actf[:, c * CHUNK : (c + 1) * CHUNK] = (gate * sigmoid(gate) * up).astype(BF16)
        h = xv[at_t, :] + dot(actf[...], wd[0]).astype(BF16)
        hv[at_t, :] = h
        wide = h.astype(F32)
        a = (wide * norm_scale(wide)).astype(BF16)
        av[at_t, :] = a
        at[:, at_t] = a.T
        dt[:, at_t] = dyv[at_t, :].T

    for copy in load_w(1):
        copy.wait()

    def compute(layer, c, i):
        w_chunk = wgu[layer, c]
        d_chunk = wd[layer, pl.ds(pl.multiple_of(c * CHUNK, CHUNK), CHUNK), :]
        for t in range(tokens // TILE):
            at_t = slice(t * TILE, (t + 1) * TILE)
            gu = dot(av[at_t, :], w_chunk)
            by_act = dot_t(dyv[at_t, :], d_chunk).astype(BF16).astype(F32)
            gate, up = gu[:, :CHUNK], gu[:, CHUNK:]
            s = sigmoid(gate)
            silu = gate * s
            act[at_t, :] = (silu * up).astype(BF16)
            dgu[at_t, :CHUNK] = (by_act * up * (s + silu * (1.0 - s))).astype(BF16)
            dgu[at_t, CHUNK:] = (by_act * silu).astype(BF16)
            if layer > 0:
                by_a = dot_t(dgu[at_t, :], w_chunk)
                acc[at_t, :] += by_a
        slot = i % TERMS
        by_gu = dot(at[...], dgu[...]).astype(BF16)
        term[slot, 0:d, :] = by_gu[:, :CHUNK]
        term[slot, d : 2 * d, :] = by_gu[:, CHUNK:]
        by_d = dot(dt[...], act[...]).T.astype(BF16)
        for n in range(d // CHUNK):
            term[slot, 2 * d + n * CHUNK : 2 * d + (n + 1) * CHUNK, :] = by_d[:, n * CHUNK : (n + 1) * CHUNK]

    def remote(src, dst, send, recv, to):
        return pltpu.make_async_remote_copy(src_ref=src, dst_ref=dst, send_sem=send, recv_sem=recv, device_id=to, device_id_type=MESH)

    def rows_at(core, chip, direction=0, count=None):
        start = core * half + chip * own + direction * piece
        return pl.ds(pl.multiple_of(start, piece), piece if count is None else count)

    def swap(j):
        there = pl.ds(pl.multiple_of(other * half, half), half)
        return remote(term.at[j % TERMS, there], from_core.at[j % HALVES], core_sem.at[0, j % SLOTS], core_sem.at[1, j % SLOTS], sibling)

    def ring(j, step, direction):
        src, dst = (run.at[j % RUNS, n, direction] for n in (step - 1, step))
        sems = (step - 1, direction, j % SLOTS)
        return remote(src, dst, ring_send.at[sems], ring_recv.at[sems], right if direction == 0 else left)

    def near(j, direction, arriving=False):
        if arriving:
            block = (chip + chips - 1) % chips if direction == 0 else (chip + 1) % chips
        else:
            block = chip
        place = g.at[j, rows_at(core, block, 0, own)]
        return remote(place, place, near_send.at[direction, j], near_recv.at[direction, j], right if direction == 0 else left)

    def far(j, direction, arriving=False):
        if arriving:
            block = (chip + 2) % chips
        else:
            block = (chip + chips - 1) % chips if direction == 0 else (chip + 1) % chips
        place = g.at[j, rows_at(core, block, direction)]
        return remote(place, place, far_send.at[direction, j], far_recv.at[direction, j], right if direction == 0 else left)

    def share(j, arriving=False):
        place = g.at[j, pl.ds(pl.multiple_of((other if arriving else core) * half, half), half)]
        return remote(place, place, half_sem.at[0, j], half_sem.at[1, j], sibling)

    def put_out(j):
        return pltpu.make_async_copy(g.at[j], g_hbm.at[pl.ds(pl.multiple_of(j * rows, rows), rows)], out_sem.at[j % SLOTS])

    def add_up(j, p, direction):
        block = (chip + 2 * chips - p) % chips if direction == 0 else (chip + p) % chips
        here = rows_at(core, block, direction)
        within = pl.ds(pl.multiple_of(block * own + direction * piece, piece), piece)
        value = term[j % TERMS, here, :].astype(F32) + from_core[j % HALVES, within, :].astype(F32)
        if p > 1:
            value = value + run[j % RUNS, p - 1, direction].astype(F32)
        value = value.astype(BF16)
        if p < chips:
            run[j % RUNS, p - 1, direction] = value
        else:
            g[j, here, :] = value
        return value

    def phases(i):
        def at_chunk(j, body):
            pl.when((j >= 0) & (j < total))(functools.partial(body, j))

        def start_swap(j):
            swap(j).start()

        def ring_phase(p, j):
            if p == 1:
                swap(j).wait()
            for direction in range(2):
                if p > 1:
                    ring(j, p - 1, direction).wait()
                value = add_up(j, p, direction)
                if p < chips:
                    ring(j, p, direction).start()
                else:
                    wide = value.astype(F32)
                    wide = jnp.sum((wide * wide).reshape(piece // 8, 8, CHUNK), 0)
                    ssq[...] += sum(wide[:, n : n + 128] for n in range(0, CHUNK, 128))
            if p == chips:
                near(j, 0).start()
                near(j, 1).start()

        def far_phase(j):
            for direction in range(2):
                near(j, direction).wait_send()
                near(j, direction, True).wait_recv()
                far(j, direction).start()

        def share_phase(j):
            for direction in range(2):
                far(j, direction).wait_send()
                far(j, direction, True).wait_recv()
            share(j).start()

        def out_phase(j):
            share(j).wait_send()
            share(j, True).wait_recv()
            put_out(j).start()

        at_chunk(i, start_swap)
        for p in range(1, chips + 1):
            at_chunk(i - p, functools.partial(ring_phase, p))
        at_chunk(i - chips - 1, far_phase)
        at_chunk(i - chips - 2, share_phase)
        at_chunk(i - chips - 3, out_phase)
        at_chunk(i - chips - 4, lambda j: put_out(j).wait())

    acc[...] = jnp.zeros_like(acc)
    ssq[...] = jnp.zeros_like(ssq)
    if COMM:
        pl.semaphore_wait(barrier, dp - 1)

    @pl.loop(0, per)
    def _(c):
        compute(1, c, c)
        if COMM:
            phases(c)

    @pl.loop(0, tokens // FTILE)
    def _(t):
        at_t = pl.ds(pl.multiple_of(t * FTILE, FTILE), FTILE)
        wide = hv[at_t, :].astype(F32)
        scale = norm_scale(wide)
        by_a = acc[at_t, :].astype(BF16).astype(F32)
        by_h = by_a * scale - wide * (scale * scale * scale * jnp.mean(by_a * wide, -1, keepdims=True))
        by_h = dyv[at_t, :] + by_h.astype(BF16)
        dyv[at_t, :] = by_h
        dt[:, at_t] = by_h.T
        wide = xv[at_t, :].astype(F32)
        a = (wide * norm_scale(wide)).astype(BF16)
        av[at_t, :] = a
        at[:, at_t] = a.T

    @pl.loop(0, per)
    def _(c):
        compute(0, c, c + per)
        if COMM:
            phases(c + per)

    if COMM:
        def to_peer(k):
            peer = (me + k) % dp
            return remote(ssq, ssq_all.at[me], ssq_send.at[k - 1], ssq_recv.at[k - 1], (rep, peer))

        def from_peer(k):
            peer = (me + dp - k) % dp
            return remote(ssq, ssq_all.at[peer], ssq_send.at[k - 1], ssq_recv.at[k - 1], (rep, peer))

        @pl.loop(total, total + chips + 1)
        def _(i):
            phases(i)

        for k in range(1, dp):
            to_peer(k).start()
        ssq_all[me] = ssq[...]

        @pl.loop(total + chips + 1, total + chips + 5)
        def _(i):
            phases(i)

        for k in range(1, dp):
            to_peer(k).wait_send()
            from_peer(k).wait_recv()
        ssq_out[...] = ssq_all[...]
    else:
        ssq_out[...] = jnp.zeros_like(ssq_out)


def gradients(x, dy, wg, wu, wd, dp):
    tokens, d = x.shape
    layers, _, ff = wg.shape
    per = ff // CHUNK
    total = layers * per
    rows = 3 * d * ff // (per * CHUNK)
    half = rows // CORES
    chips = dp // CORES
    dma = pltpu.SemaphoreType.DMA
    return pl.pallas_call(
        functools.partial(grad_kernel, dp, layers),
        out_shape=(
            jax.ShapeDtypeStruct((total * rows, CHUNK), BF16),
            jax.ShapeDtypeStruct((dp, 8, 128), F32),
        ),
        in_specs=[pl.BlockSpec(memory_space=pl.ANY)] * 5,
        out_specs=(pl.BlockSpec(memory_space=pl.ANY), pl.BlockSpec(memory_space=pltpu.VMEM)),
        scratch_shapes=[
            pltpu.VMEM((tokens, d), BF16),
            pltpu.VMEM((tokens, d), BF16),
            pltpu.VMEM((tokens, d), BF16),
            pltpu.VMEM((tokens, d), BF16),
            pltpu.VMEM((d, tokens), BF16),
            pltpu.VMEM((d, tokens), BF16),
            pltpu.VMEM((tokens, d), F32),
            pltpu.VMEM((FTILE, ff), BF16),
            pltpu.VMEM((tokens, CHUNK), BF16),
            pltpu.VMEM((tokens, 2 * CHUNK), BF16),
            pltpu.VMEM((layers, per, d, 2 * CHUNK), BF16),
            pltpu.VMEM((layers, ff, d), BF16),
            pltpu.VMEM((TERMS, rows, CHUNK), BF16),
            pltpu.VMEM((HALVES, half, CHUNK), BF16),
            pltpu.VMEM((RUNS, chips, 2, half // chips // 2, CHUNK), BF16),
            pltpu.VMEM((total, rows, CHUNK), BF16),
            pltpu.VMEM((8, 128), F32),
            pltpu.VMEM((dp, 8, 128), F32),
            dma((2,)),
            dma((layers, per, 3)),
            dma((SLOTS,)),
            dma((2, SLOTS)),
            dma((chips - 1, 2, SLOTS)),
            dma((chips - 1, 2, SLOTS)),
            dma((2, total)),
            dma((2, total)),
            dma((2, total)),
            dma((2, total)),
            dma((2, total)),
            dma((dp - 1,)),
            dma((dp - 1,)),
        ],
        compiler_params=pltpu.CompilerParams(collective_id=0, has_side_effects=True, vmem_limit_bytes=67043328),
        name="gradients",
    )(x, dy, wg, wu, wd)


def adamw_kernel(count, ssq, g, *refs):
    ins, outs = refs[:9], refs[9:]
    d = ins[0].shape[1]
    mean = jnp.sum(jnp.sum(ssq[...], 0), keepdims=True) / count
    factor = jnp.minimum(1.0, 0.5 * lax.rsqrt(mean + 1e-30))

    def one(n, index, piece):
        w, m, v = (ins[n + 3 * k] for k in range(3))
        new_w, new_m, new_v = (outs[n + 3 * k] for k in range(3))
        grad = piece.astype(F32) * factor
        wide = w[index].astype(F32)
        m1 = 0.9 * m[index] + 0.1 * grad
        v1 = 0.95 * v[index] + 0.05 * grad * grad
        new_m[index] = m1
        new_v[index] = v1
        new_w[index] = (wide - 0.02 * (m1 * lax.rsqrt(v1 + 1e-8) + 0.1 * wide)).astype(BF16)

    one(0, (0,), g[0:d, :])
    one(1, (0,), g[d : 2 * d, :])
    for n in range(d // CHUNK):
        one(2, (0, slice(None), slice(n * CHUNK, (n + 1) * CHUNK)), g[2 * d + n * CHUNK : 2 * d + (n + 1) * CHUNK, :])


def adamw(ssq, g, weights, m, v):
    layers, d, ff = weights[0].shape
    per = ff // CHUNK
    rows = g.shape[0] // (layers * per)
    wide = pl.BlockSpec((1, d, CHUNK), lambda l, c: (l, 0, c))
    tall = pl.BlockSpec((1, CHUNK, d), lambda l, c: (l, c, 0))
    trio = [wide, wide, tall]
    count = sum(w.size for w in weights)
    return pl.pallas_call(
        functools.partial(adamw_kernel, count),
        grid=(layers, per),
        out_shape=tuple(jax.ShapeDtypeStruct(a.shape, a.dtype) for a in (*weights, *m, *v)),
        in_specs=[
            pl.BlockSpec(ssq.shape, lambda l, c: (0, 0, 0)),
            pl.BlockSpec((rows, CHUNK), lambda l, c: ((layers - 1 - l) * per + c, 0)),
            *trio, *trio, *trio,
        ],
        out_specs=tuple(trio * 3),
        compiler_params=pltpu.CompilerParams(vmem_limit_bytes=48 * 2**20),
        name="adamw",
    )(ssq, g, *weights, *m, *v)


def solution(mesh):
    dp = mesh.shape["dp"]

    def step(x, dy, *arrays):
        weights, m, v = (arrays[i : i + 3] for i in (0, 3, 6))
        g, ssq = gradients(x[0], dy[0], *weights, dp)
        return adamw(ssq, g, weights, m, v)

    return jax.shard_map(
        step,
        mesh=mesh,
        in_specs=(P(("rep", "dp"), None, None),) * 2 + (P(None, None, None),) * 9,
        out_specs=(P("rep", None, None),) * 9,
        check_vma=False,
    )
```

```python
import functools

import jax
import jax.numpy as jnp
from jax import lax
from jax.experimental import pallas as pl
from jax.experimental.pallas import tpu as pltpu
from jax.sharding import PartitionSpec as P

MESH = pl.DeviceIdType.MESH
BF16, F32 = jnp.bfloat16, jnp.float32
CORES = 2
CHUNK = 256
TILE = 512
FTILE = 256
LAG = 1
GATHER_LAG = 2
STEPS = 4
SLOTS = 2 * LAG + 2
TERMS = STEPS * LAG + 1
HALVES = (STEPS + 1) * LAG + 2
RUNS = STEPS * LAG + 2
PART = 8
LATE = 8
COMM = True


def dot(a, b):
    return jnp.dot(a, b, preferred_element_type=F32)


def dot_t(a, b):
    return lax.dot_general(a, b, (((1,), (1,)), ((), ())), preferred_element_type=F32)


def sigmoid(z):
    return 0.5 * jnp.tanh(0.5 * z) + 0.5


def norm_scale(wide):
    return lax.rsqrt(jnp.mean(wide * wide, -1, keepdims=True) + 1e-6)


def grad_kernel(
    dp, layers, x_hbm, dy_hbm, wg_hbm, wu_hbm, wd_hbm, g_hbm, mine_hbm, ssq_out,
    xv, dyv, hv, av, at, dt, acc, actf, act, dgu, wgu, wd, term, from_core, run, g, mine, ssq, ssq_all,
    io_sem, w_sem, out_sem, mine_sem, core_sem, ring_send, ring_recv, near_send, near_recv, far_send, far_recv, half_sem, ssq_send, ssq_recv,
):
    tokens, d = xv.shape
    ff = wd_hbm.shape[1]
    per = ff // CHUNK
    total = layers * per
    chips = dp // CORES
    early = total - LATE
    rows = g.shape[1]
    half = rows // CORES
    own = half // chips
    piece = own // 2
    rep = lax.axis_index("rep")
    me = lax.axis_index("dp")
    chip, core = me // CORES, me % CORES
    other = 1 - core

    def device(chip, core):
        return (rep, chip * CORES + core)

    right, left = device((chip + 1) % chips, core), device((chip + chips - 1) % chips, core)
    sibling = device(chip, other)

    barrier = pltpu.get_barrier_semaphore()
    if COMM:
        for k in range(1, dp):
            pl.semaphore_signal(barrier, inc=1, device_id=(rep, (me + k) % dp), device_id_type=MESH)

    def load_x():
        return pltpu.make_async_copy(x_hbm, xv, io_sem.at[0])

    def load_dy():
        return pltpu.make_async_copy(dy_hbm, dyv, io_sem.at[1])

    def load_w(layer):
        copies = []
        for c in range(per):
            cut = slice(c * CHUNK, (c + 1) * CHUNK)
            copies.append(pltpu.make_async_copy(wg_hbm.at[layer, :, cut], wgu.at[layer, c, :, :CHUNK], w_sem.at[layer, c, 0]))
            copies.append(pltpu.make_async_copy(wu_hbm.at[layer, :, cut], wgu.at[layer, c, :, CHUNK:], w_sem.at[layer, c, 1]))
            copies.append(pltpu.make_async_copy(wd_hbm.at[layer, cut, :], wd.at[layer, cut, :], w_sem.at[layer, c, 2]))
        return copies

    load_x().start()
    for copy in load_w(0):
        copy.start()
    load_dy().start()
    for copy in load_w(1):
        copy.start()

    load_x().wait()
    for copy in load_w(0):
        copy.wait()
    load_dy().wait()

    @pl.loop(0, tokens // FTILE)
    def _(t):
        at_t = pl.ds(pl.multiple_of(t * FTILE, FTILE), FTILE)
        wide = xv[at_t, :].astype(F32)
        a = (wide * norm_scale(wide)).astype(BF16)
        for c in range(per):
            gu = dot(a, wgu[0, c])
            gate, up = gu[:, :CHUNK], gu[:, CHUNK:]
            actf[:, c * CHUNK : (c + 1) * CHUNK] = (gate * sigmoid(gate) * up).astype(BF16)
        h = xv[at_t, :] + dot(actf[...], wd[0]).astype(BF16)
        hv[at_t, :] = h
        wide = h.astype(F32)
        a = (wide * norm_scale(wide)).astype(BF16)
        av[at_t, :] = a
        at[:, at_t] = a.T
        dt[:, at_t] = dyv[at_t, :].T

    for copy in load_w(1):
        copy.wait()

    def compute(layer, c, i):
        w_chunk = wgu[layer, c]
        d_chunk = wd[layer, pl.ds(pl.multiple_of(c * CHUNK, CHUNK), CHUNK), :]
        for t in range(tokens // TILE):
            at_t = slice(t * TILE, (t + 1) * TILE)
            gu = dot(av[at_t, :], w_chunk)
            by_act = dot_t(dyv[at_t, :], d_chunk).astype(BF16).astype(F32)
            gate, up = gu[:, :CHUNK], gu[:, CHUNK:]
            s = sigmoid(gate)
            silu = gate * s
            act[at_t, :] = (silu * up).astype(BF16)
            dgu[at_t, :CHUNK] = (by_act * up * (s + silu * (1.0 - s))).astype(BF16)
            dgu[at_t, CHUNK:] = (by_act * silu).astype(BF16)
            if layer > 0:
                by_a = dot_t(dgu[at_t, :], w_chunk)
                acc[at_t, :] += by_a
        slot = i % TERMS
        by_gu = dot(at[...], dgu[...]).astype(BF16)
        by_d = dot(dt[...], act[...]).T.astype(BF16)
        blocks = rows // piece
        n, m = d // blocks, CHUNK // blocks
        for b in range(blocks):
            start = b * piece
            term[slot, start : start + n, :] = by_gu[b * n : (b + 1) * n, :CHUNK]
            term[slot, start + n : start + 2 * n, :] = by_gu[b * n : (b + 1) * n, CHUNK:]
            for k in range(d // CHUNK):
                low = start + 2 * n + k * m
                term[slot, low : low + m, :] = by_d[b * m : (b + 1) * m, k * CHUNK : (k + 1) * CHUNK]

    def remote(src, dst, send, recv, to):
        return pltpu.make_async_remote_copy(src_ref=src, dst_ref=dst, send_sem=send, recv_sem=recv, device_id=to, device_id_type=MESH)

    def rows_at(core, chip, direction=0, count=None):
        start = core * half + chip * own + direction * piece
        return pl.ds(pl.multiple_of(start, piece), piece if count is None else count)

    def swap(j):
        there = pl.ds(pl.multiple_of(other * half, half), half)
        return remote(term.at[j % TERMS, there], from_core.at[j % HALVES], core_sem.at[0, j % SLOTS], core_sem.at[1, j % SLOTS], sibling)

    def ring(j, step, direction):
        src, dst = (run.at[j % RUNS, n, direction] for n in (step - 1, step))
        sems = (step - 1, direction, j % SLOTS)
        return remote(src, dst, ring_send.at[sems], ring_recv.at[sems], right if direction == 0 else left)

    def near(j, direction, arriving=False):
        if arriving:
            block = (chip + chips - 1) % chips if direction == 0 else (chip + 1) % chips
        else:
            block = chip
        place = g.at[j, rows_at(core, block, 0, own)]
        return remote(place, place, near_send.at[direction, j], near_recv.at[direction, j], right if direction == 0 else left)

    def far(j, direction, arriving=False):
        if arriving:
            block = (chip + 2) % chips
        else:
            block = (chip + chips - 1) % chips if direction == 0 else (chip + 1) % chips
        place = g.at[j, rows_at(core, block, direction)]
        return remote(place, place, far_send.at[direction, j], far_recv.at[direction, j], right if direction == 0 else left)

    def share(j, arriving=False):
        place = g.at[j, pl.ds(pl.multiple_of((other if arriving else core) * half, half), half)]
        return remote(place, place, half_sem.at[0, j], half_sem.at[1, j], sibling)

    def put_out(j):
        return pltpu.make_async_copy(g.at[j], g_hbm.at[j], out_sem.at[j % SLOTS])

    def put_mine():
        return pltpu.make_async_copy(mine, mine_hbm, mine_sem)

    def add_up(j, p, direction):
        block = (chip + 2 * chips - p) % chips if direction == 0 else (chip + p) % chips
        here = rows_at(core, block, direction)
        within = pl.ds(pl.multiple_of(block * own + direction * piece, piece), piece)
        value = term[j % TERMS, here, :].astype(F32) + from_core[j % HALVES, within, :].astype(F32)
        if p > 1:
            value = value + run[j % RUNS, p - 1, direction].astype(F32)
        value = value.astype(BF16)
        if p < chips:
            run[j % RUNS, p - 1, direction] = value
        else:
            @pl.when(j < early)
            def _():
                g[j, here, :] = value

            @pl.when(j >= early)
            def _():
                mine[jnp.maximum(j - early, 0), direction * piece : (direction + 1) * piece, :] = value

        return value

    def phases(i):
        def at_chunk(j, body, end=total):
            pl.when((j >= 0) & (j < end))(functools.partial(body, j))

        def start_swap(j):
            swap(j).start()

        def ring_phase(p, j):
            if p == 1:
                swap(j).wait()
            for direction in range(2):
                if p > 1:
                    ring(j, p - 1, direction).wait()
                value = add_up(j, p, direction)
                if p < chips:
                    ring(j, p, direction).start()
                else:
                    wide = value.astype(F32)
                    wide = jnp.sum((wide * wide).reshape(piece // 8, 8, CHUNK), 0)
                    ssq[...] += sum(wide[:, n : n + 128] for n in range(0, CHUNK, 128))
            if p == chips:
                @pl.when(j < early)
                def _():
                    near(j, 0).start()
                    near(j, 1).start()

        def far_phase(j):
            for direction in range(2):
                near(j, direction).wait_send()
                near(j, direction, True).wait_recv()
                far(j, direction).start()

        def share_phase(j):
            for direction in range(2):
                far(j, direction).wait_send()
                far(j, direction, True).wait_recv()
            share(j).start()

        def out_phase(j):
            share(j).wait_send()
            share(j, True).wait_recv()
            put_out(j).start()

        at_chunk(i, start_swap)
        for p in range(1, chips + 1):
            at_chunk(i - LAG * p, functools.partial(ring_phase, p))
        at_chunk(i - LAG * chips - GATHER_LAG, far_phase, early)
        at_chunk(i - LAG * chips - 2 * GATHER_LAG, share_phase, early)
        at_chunk(i - LAG * chips - 3 * GATHER_LAG, out_phase, early)
        at_chunk(i - LAG * chips - 3 * GATHER_LAG - 1, lambda j: put_out(j).wait(), early)

    acc[...] = jnp.zeros_like(acc)
    ssq[...] = jnp.zeros_like(ssq)
    if COMM:
        pl.semaphore_wait(barrier, dp - 1)

    @pl.loop(0, per)
    def _(c):
        compute(1, c, c)
        if COMM:
            phases(c)

    @pl.loop(0, tokens // FTILE)
    def _(t):
        at_t = pl.ds(pl.multiple_of(t * FTILE, FTILE), FTILE)
        wide = hv[at_t, :].astype(F32)
        scale = norm_scale(wide)
        by_a = acc[at_t, :].astype(BF16).astype(F32)
        by_h = by_a * scale - wide * (scale * scale * scale * jnp.mean(by_a * wide, -1, keepdims=True))
        by_h = dyv[at_t, :] + by_h.astype(BF16)
        dyv[at_t, :] = by_h
        dt[:, at_t] = by_h.T
        wide = xv[at_t, :].astype(F32)
        a = (wide * norm_scale(wide)).astype(BF16)
        av[at_t, :] = a
        at[:, at_t] = a.T

    @pl.loop(0, per)
    def _(c):
        compute(0, c, c + per)
        if COMM:
            phases(c + per)

    if COMM:
        def to_peer(k):
            peer = (me + k) % dp
            return remote(ssq, ssq_all.at[me], ssq_send.at[k - 1], ssq_recv.at[k - 1], (rep, peer))

        def from_peer(k):
            peer = (me + dp - k) % dp
            return remote(ssq, ssq_all.at[peer], ssq_send.at[k - 1], ssq_recv.at[k - 1], (rep, peer))

        @pl.loop(total, total + LAG * chips)
        def _(i):
            phases(i)

        for k in range(1, dp):
            to_peer(k).start()
        ssq_all[me] = ssq[...]
        put_mine().start()
        for i in range(total + LAG * chips, early + LAG * chips + 3 * GATHER_LAG + 1):
            phases(i)
        for k in range(1, dp):
            to_peer(k).wait_send()
            from_peer(k).wait_recv()
        ssq_out[...] = ssq_all[...]
        put_mine().wait()
    else:
        ssq_out[...] = jnp.zeros_like(ssq_out)


def gradients(x, dy, wg, wu, wd, dp):
    tokens, d = x.shape
    layers, _, ff = wg.shape
    per = ff // CHUNK
    total = layers * per
    rows = 3 * d * ff // (per * CHUNK)
    half = rows // CORES
    chips = dp // CORES
    dma = pltpu.SemaphoreType.DMA
    return pl.pallas_call(
        functools.partial(grad_kernel, dp, layers),
        out_shape=(
            jax.ShapeDtypeStruct((total - LATE, rows, CHUNK), BF16),
            jax.ShapeDtypeStruct((LATE, rows // dp, CHUNK), BF16),
            jax.ShapeDtypeStruct((dp, 8, 128), F32),
        ),
        in_specs=[pl.BlockSpec(memory_space=pl.ANY)] * 5,
        out_specs=(pl.BlockSpec(memory_space=pl.ANY), pl.BlockSpec(memory_space=pl.ANY), pl.BlockSpec(memory_space=pltpu.VMEM)),
        scratch_shapes=[
            pltpu.VMEM((tokens, d), BF16),
            pltpu.VMEM((tokens, d), BF16),
            pltpu.VMEM((tokens, d), BF16),
            pltpu.VMEM((tokens, d), BF16),
            pltpu.VMEM((d, tokens), BF16),
            pltpu.VMEM((d, tokens), BF16),
            pltpu.VMEM((tokens, d), F32),
            pltpu.VMEM((FTILE, ff), BF16),
            pltpu.VMEM((tokens, CHUNK), BF16),
            pltpu.VMEM((tokens, 2 * CHUNK), BF16),
            pltpu.VMEM((layers, per, d, 2 * CHUNK), BF16),
            pltpu.VMEM((layers, ff, d), BF16),
            pltpu.VMEM((TERMS, rows, CHUNK), BF16),
            pltpu.VMEM((HALVES, half, CHUNK), BF16),
            pltpu.VMEM((RUNS, chips, 2, half // chips // 2, CHUNK), BF16),
            pltpu.VMEM((total - LATE, rows, CHUNK), BF16),
            pltpu.VMEM((LATE, rows // dp, CHUNK), BF16),
            pltpu.VMEM((8, 128), F32),
            pltpu.VMEM((dp, 8, 128), F32),
            dma((2,)),
            dma((layers, per, 3)),
            dma((SLOTS,)),
            dma,
            dma((2, SLOTS)),
            dma((chips - 1, 2, SLOTS)),
            dma((chips - 1, 2, SLOTS)),
            dma((2, total)),
            dma((2, total)),
            dma((2, total)),
            dma((2, total)),
            dma((2, total)),
            dma((dp - 1,)),
            dma((dp - 1,)),
        ],
        compiler_params=pltpu.CompilerParams(collective_id=0, has_side_effects=True, vmem_limit_bytes=67043328),
        name="gradients",
    )(x, dy, wg, wu, wd)


def adamw_kernel(count, n_g, n_old, ids, ssq, *refs):
    gs, ins, outs = refs[:n_g], refs[n_g : n_g + 9], refs[n_g + 9 + n_old :]
    mean = jnp.sum(jnp.sum(ssq[...], 0), keepdims=True) / count
    factor = jnp.minimum(1.0, 0.5 * lax.rsqrt(mean + 1e-30))

    def grad(chunk, rows):
        if n_g == 1:
            return gs[0][0, chunk, rows, :].astype(F32) * factor
        value = gs[0][chunk, rows, :]
        for k in range(1, n_g):
            value = jnp.where(pl.program_id(0) == k, gs[k][chunk, rows, :], value)
        return value.astype(F32) * factor

    def one(n, index, grad):
        w, m, v = (ins[n + 3 * k] for k in range(3))
        new_w, new_m, new_v = (outs[n + 3 * k] for k in range(3))
        wide = w[index].astype(F32)
        m1 = 0.9 * m[index] + 0.1 * grad
        v1 = 0.95 * v[index] + 0.05 * grad * grad
        new_m[index] = m1
        new_v[index] = v1
        new_w[index] = (wide - 0.02 * (m1 * lax.rsqrt(v1 + 1e-8) + 0.1 * wide)).astype(BF16)

    wide_rows, d = ins[0].shape[1] // 2, ins[2].shape[4]
    tall_rows = ins[2].shape[3] // 2
    for chunk in range(PART):
        for direction in range(2):
            start = direction * (2 * wide_rows + d // CHUNK * tall_rows)
            there = (0, slice(direction * wide_rows, (direction + 1) * wide_rows), slice(chunk * CHUNK, (chunk + 1) * CHUNK))
            one(0, there, grad(chunk, slice(start, start + wide_rows)))
            one(1, there, grad(chunk, slice(start + wide_rows, start + 2 * wide_rows)))
            for k in range(d // CHUNK):
                low = start + 2 * wide_rows + k * tall_rows
                there = (0, 0, chunk, slice(direction * tall_rows, (direction + 1) * tall_rows), slice(k * CHUNK, (k + 1) * CHUNK))
                one(2, there, grad(chunk, slice(low, low + tall_rows)))


def adamw(dp, count, ids, ssq, gs, arrays, first_part, order, first_id=0, old=None):
    layers, d, ff = arrays[0].shape
    per = ff // CHUNK // PART

    def layer(p):
        return layers - 1 - p // per

    if len(gs) == 1:
        grid = (dp,)

        def place(i, ids):
            return first_part, i

        g_specs = [pl.BlockSpec((1, PART, gs[0].shape[2] // dp, CHUNK), lambda i, ids: (first_part, 0, i, 0))]
    else:
        grid = (len(gs),)

        def place(i, ids):
            return first_part, ids[first_id + i]

        g_specs = [pl.BlockSpec(g.shape, lambda i, ids: (0, 0, 0)) for g in gs]

    def wide_index(i, ids):
        p, s = place(i, ids)
        return layer(p), s, p % per

    def tall_index(i, ids):
        p, s = place(i, ids)
        return layer(p), p % per, 0, s, 0

    wide = pl.BlockSpec((1, d // dp, PART * CHUNK), wide_index)
    tall = pl.BlockSpec((1, 1, PART, CHUNK // dp, d), tall_index)
    trio = [wide, wide, tall]
    old = old or ()
    first_old = 2 + len(gs) + 9
    elements = grid[0] * PART * 3 * d * CHUNK // dp
    return pl.pallas_call(
        functools.partial(adamw_kernel, count, len(gs), len(old)),
        out_shape=tuple(jax.ShapeDtypeStruct(a.shape, a.dtype) for a in arrays),
        grid_spec=pltpu.PrefetchScalarGridSpec(
            num_scalar_prefetch=1,
            grid=grid,
            in_specs=[
                pl.BlockSpec(ssq.shape, lambda i, ids: (0, 0, 0)),
                *g_specs, *trio, *trio, *trio,
                *[pl.BlockSpec(memory_space=pl.ANY)] * len(old),
            ],
            out_specs=tuple(trio * 3),
        ),
        input_output_aliases={first_old + n: n for n in range(len(old))},
        compiler_params=pltpu.CompilerParams(vmem_limit_bytes=60 * 2**20),
        cost_estimate=pl.CostEstimate(flops=elements * 40, bytes_accessed=elements * 22, transcendentals=elements),
        name=f"adamw{order}",
    )(ids, ssq, *gs, *arrays, *old)


def solution(mesh):
    dp = mesh.shape["dp"]
    chips = dp // CORES

    def step(x, dy, *arrays):
        weights = arrays[:3]
        layers, d, ff = weights[0].shape
        count = sum(w.size for w in weights)
        me = lax.axis_index("dp")
        chip, core = me // CORES, me % CORES
        turn = 1 - 2 * core
        behind, ahead, far = ((chip + chips + n) % chips for n in (-turn, turn, chips // 2))
        ids = jnp.stack([k * chips + c for k, c in (
            (core, chip), (1 - core, chip), (core, behind), (core, ahead),
            (1 - core, ahead), (1 - core, behind), (core, far), (1 - core, far),
        )])

        def index(chip, core):
            return chip % chips * CORES + core

        devices = [(c, k) for c in range(chips) for k in range(CORES)]
        on = [(index(c, k), index(c + 1 - 2 * k, k)) for c, k in devices]
        back = [(b, a) for a, b in on]
        over = [(index(c, k), index(c, 1 - k)) for c, k in devices]
        on_over = [(index(c, k), index(c + 1 - 2 * k, 1 - k)) for c, k in devices]

        g, mine, ssq = gradients(x[0], dy[0], *weights, dp)
        arrays = [a.reshape(layers, -1, PART, CHUNK, d) if n % 3 == 2 else a for n, a in enumerate(arrays)]
        g = g.reshape(-1, PART, *g.shape[1:])
        update = functools.partial(adamw, dp, count, ids, ssq)
        mine_over = lax.ppermute(mine, "dp", over)
        one = lax.ppermute(mine, "dp", on)
        two = lax.ppermute(mine, "dp", back)
        new = update([g], arrays, 0, 0)
        one, two, mine_over, new = lax.optimization_barrier((one, two, mine_over, new))
        far = lax.ppermute(one, "dp", on)
        far_over = lax.ppermute(one, "dp", on_over)
        one_over = lax.ppermute(one, "dp", over)
        two_over = lax.ppermute(two, "dp", over)
        new = update([mine, mine_over, one, two], arrays, 1, 1, 0, new)
        one_over, two_over, far, far_over, new = lax.optimization_barrier((one_over, two_over, far, far_over, new))
        new = update([one_over, two_over, far, far_over], arrays, 1, 2, 4, new)
        return tuple(a.reshape(layers, ff, d) if n % 3 == 2 else a for n, a in enumerate(new))

    return jax.shard_map(
        step,
        mesh=mesh,
        in_specs=(P(("rep", "dp"), None, None),) * 2 + (P(None, None, None),) * 9,
        out_specs=(P("rep", None, None),) * 9,
        check_vma=False,
    )
```

```python
import functools

import jax
import jax.numpy as jnp
from jax import lax
from jax.experimental import pallas as pl
from jax.experimental.pallas import tpu as pltpu
from jax.sharding import PartitionSpec as P

MESH = pl.DeviceIdType.MESH
BF16, F32 = jnp.bfloat16, jnp.float32
CORES = 2
CHUNK = 256
TILE = 1024
FTILE = 256
LAG = 1
GATHER_LAG = 2
STEPS = 3
SLOTS = STEPS * LAG + 2
TERMS = STEPS * LAG + 1
HALVES = (STEPS + 1) * LAG + 2
RUNS = STEPS * LAG + 2
PART = 8
FIRST = 5
LATE = 8
COMM = True


def dot(a, b):
    return jnp.dot(a, b, preferred_element_type=F32)


def dot_t(a, b):
    return lax.dot_general(a, b, (((1,), (1,)), ((), ())), preferred_element_type=F32)


def sigmoid(z):
    return 0.5 * jnp.tanh(0.5 * z) + 0.5


def norm_scale(wide):
    return lax.rsqrt(jnp.mean(wide * wide, -1, keepdims=True) + 1e-6)


def grad_kernel(
    dp, layers, x_hbm, dy_hbm, wg_hbm, wu_hbm, wd_hbm, g_hbm, mine_hbm, ssq_out,
    xv, dyv, hv, av, at, acc, actf, act, by_next, dgu, wgu, wd, term, from_core, leaving, coming, g, mine, ssq, ssq_all,
    io_sem, w_sem, out_sem, mine_sem, core_sem, ring_send, ring_recv, near_send, near_recv, far_send, far_recv, half_sem, ssq_send, ssq_recv,
):
    tokens, d = xv.shape
    ff = wd_hbm.shape[1]
    per = ff // CHUNK
    total = layers * per
    chips = dp // CORES
    early = total - LATE
    rows = g.shape[1]
    half = rows // CORES
    own = half // chips
    piece = own // 2
    rep = lax.axis_index("rep")
    me = lax.axis_index("dp")
    chip, core = me // CORES, me % CORES
    other = 1 - core

    def device(chip, core):
        return (rep, chip * CORES + core)

    right, left = device((chip + 1) % chips, core), device((chip + chips - 1) % chips, core)
    sibling = device(chip, other)

    barrier = pltpu.get_barrier_semaphore()
    if COMM:
        for k in range(1, dp):
            pl.semaphore_signal(barrier, inc=1, device_id=(rep, (me + k) % dp), device_id_type=MESH)

    def load_x():
        return pltpu.make_async_copy(x_hbm, xv, io_sem.at[0])

    def load_dy():
        return pltpu.make_async_copy(dy_hbm, dyv, io_sem.at[1])

    def load_w(layer):
        copies = []
        for c in range(per):
            cut = slice(c * CHUNK, (c + 1) * CHUNK)
            copies.append(pltpu.make_async_copy(wg_hbm.at[layer, :, cut], wgu.at[layer, c, :, :CHUNK], w_sem.at[layer, c, 0]))
            copies.append(pltpu.make_async_copy(wu_hbm.at[layer, :, cut], wgu.at[layer, c, :, CHUNK:], w_sem.at[layer, c, 1]))
            copies.append(pltpu.make_async_copy(wd_hbm.at[layer, cut, :], wd.at[layer, cut, :], w_sem.at[layer, c, 2]))
        return copies

    load_x().start()
    for copy in load_w(0):
        copy.start()
    load_dy().start()
    for copy in load_w(1):
        copy.start()

    load_x().wait()
    for copy in load_w(0):
        copy.wait()
    load_dy().wait()

    @pl.loop(0, tokens // FTILE)
    def _(t):
        at_t = pl.ds(pl.multiple_of(t * FTILE, FTILE), FTILE)
        wide = xv[at_t, :].astype(F32)
        a = (wide * norm_scale(wide)).astype(BF16)
        for c in range(per):
            gu = dot(a, wgu[0, c])
            gate, up = gu[:, :CHUNK], gu[:, CHUNK:]
            actf[:, c * CHUNK : (c + 1) * CHUNK] = (gate * sigmoid(gate) * up).astype(BF16)
        h = xv[at_t, :] + dot(actf[...], wd[0]).astype(BF16)
        hv[at_t, :] = h
        wide = h.astype(F32)
        a = (wide * norm_scale(wide)).astype(BF16)
        av[at_t, :] = a
        at[:, at_t] = a.T

    for copy in load_w(1):
        copy.wait()

    def compute(layer, c, i, second):
        w_chunk = wgu[layer, c]
        for t in range(tokens // TILE):
            at_t = slice(t * TILE, (t + 1) * TILE)
            gu = dot(av[at_t, :], w_chunk)
            if second:
                by_act = by_next[at_t, :].astype(F32)
            else:
                both = dot_t(dyv[at_t, :], wd[layer, pl.ds(pl.multiple_of(c * CHUNK, 2 * CHUNK), 2 * CHUNK), :]).astype(BF16)
                by_act = both[:, :CHUNK].astype(F32)
                by_next[at_t, :] = both[:, CHUNK:]
            gate, up = gu[:, :CHUNK], gu[:, CHUNK:]
            s = sigmoid(gate)
            silu = gate * s
            act[at_t, :] = (silu * up).astype(BF16)
            dgu[at_t, :CHUNK] = (by_act * up * (s + silu * (1.0 - s))).astype(BF16)
            dgu[at_t, CHUNK:] = (by_act * silu).astype(BF16)
            if layer > 0:
                by_a = dot_t(dgu[at_t, :], w_chunk)
                acc[at_t, :] += by_a
        slot = i % TERMS
        by_gu = dot(at[...], dgu[...]).astype(BF16)
        by_d = lax.dot_general(act[...], dyv[...], (((0,), (0,)), ((), ())), preferred_element_type=F32).astype(BF16)
        blocks = rows // piece
        n, m = d // blocks, CHUNK // blocks
        for b in range(blocks):
            start = b * piece
            term[slot, start : start + n, :] = by_gu[b * n : (b + 1) * n, :CHUNK]
            term[slot, start + n : start + 2 * n, :] = by_gu[b * n : (b + 1) * n, CHUNK:]
            for k in range(d // CHUNK):
                low = start + 2 * n + k * m
                term[slot, low : low + m, :] = by_d[b * m : (b + 1) * m, k * CHUNK : (k + 1) * CHUNK]

    def remote(src, dst, send, recv, to):
        return pltpu.make_async_remote_copy(src_ref=src, dst_ref=dst, send_sem=send, recv_sem=recv, device_id=to, device_id_type=MESH)

    def rows_at(core, chip, direction=0, count=None):
        start = core * half + chip * own + direction * piece
        return pl.ds(pl.multiple_of(start, piece), piece if count is None else count)

    def swap(j):
        there = pl.ds(pl.multiple_of(other * half, half), half)
        return remote(term.at[j % TERMS, there], from_core.at[j % HALVES], core_sem.at[0, j % SLOTS], core_sem.at[1, j % SLOTS], sibling)

    def travel(j, k):
        src = leaving.at[j % RUNS, k] if k < 4 else coming.at[j % RUNS, k - 4]
        return remote(src, coming.at[j % RUNS, k], ring_send.at[k, j % SLOTS], ring_recv.at[k, j % SLOTS], right if k % 2 == 0 else left)

    def near(j, direction, arriving=False):
        if arriving:
            block = (chip + chips - 1) % chips if direction == 0 else (chip + 1) % chips
        else:
            block = chip
        place = g.at[j, rows_at(core, block, 0, own)]
        return remote(place, place, near_send.at[direction, j], near_recv.at[direction, j], right if direction == 0 else left)

    def far(j, direction, arriving=False):
        if arriving:
            block = (chip + 2) % chips
        else:
            block = (chip + chips - 1) % chips if direction == 0 else (chip + 1) % chips
        place = g.at[j, rows_at(core, block, direction)]
        return remote(place, place, far_send.at[direction, j], far_recv.at[direction, j], right if direction == 0 else left)

    def share(j, arriving=False):
        place = g.at[j, pl.ds(pl.multiple_of((other if arriving else core) * half, half), half)]
        return remote(place, place, half_sem.at[0, j], half_sem.at[1, j], sibling)

    def put_out(j):
        return pltpu.make_async_copy(g.at[j], g_hbm.at[j], out_sem.at[j % SLOTS])

    def put_mine():
        return pltpu.make_async_copy(mine, mine_hbm, mine_sem)

    def add_up(j, turn, direction, arrived=()):
        block = (chip + turn) % chips
        here = rows_at(core, block, direction)
        within = pl.ds(pl.multiple_of(block * own + direction * piece, piece), piece)
        value = term[j % TERMS, here, :].astype(F32) + from_core[j % HALVES, within, :].astype(F32)
        for k in arrived:
            value = value + coming[j % RUNS, k].astype(F32)
        return value.astype(BF16)

    def phases(i):
        def at_chunk(j, body, end=total):
            pl.when((j >= 0) & (j < end))(functools.partial(body, j))

        def start_swap(j):
            swap(j).start()

        def through(j):
            swap(j).wait()
            for k in range(2):
                leaving[j % RUNS, k] = add_up(j, chips // 2, k)
                travel(j, k).start()

        def onward(j):
            for k in range(2):
                travel(j, k).wait()
                coming[j % RUNS, k] = add_up(j, 1 if k == 0 else chips - 1, k, (k,))
                travel(j, k + 4).start()

        def alone(j):
            for k in range(2, 4):
                leaving[j % RUNS, k] = add_up(j, 1 if k == 2 else chips - 1, 3 - k)
                travel(j, k).start()

        def finish(j):
            for k in range(2, 6):
                travel(j, k).wait()
            for direction in range(2):
                value = add_up(j, 0, direction, (3 - direction, 4 + direction))
                wide = value.astype(F32)
                wide = jnp.sum((wide * wide).reshape(piece // 8, 8, CHUNK), 0)
                ssq[...] += sum(wide[:, n : n + 128] for n in range(0, CHUNK, 128))

                @pl.when(j < early)
                def _():
                    g[j, rows_at(core, chip, direction), :] = value

                @pl.when(j >= early)
                def _():
                    mine[jnp.maximum(j - early, 0), direction * piece : (direction + 1) * piece, :] = value

            @pl.when(j < early)
            def _():
                near(j, 0).start()
                near(j, 1).start()

        def far_phase(j):
            for direction in range(2):
                near(j, direction).wait_send()
                near(j, direction, True).wait_recv()
                far(j, direction).start()

        def share_phase(j):
            for direction in range(2):
                far(j, direction).wait_send()
                far(j, direction, True).wait_recv()
            share(j).start()

        def out_phase(j):
            share(j).wait_send()
            share(j, True).wait_recv()
            put_out(j).start()

        at_chunk(i, start_swap)
        at_chunk(i - LAG, through)
        at_chunk(i - 2 * LAG, onward)
        at_chunk(i - LAG, alone)
        at_chunk(i - 3 * LAG, finish)
        at_chunk(i - LAG * STEPS - GATHER_LAG, far_phase, early)
        at_chunk(i - LAG * STEPS - 2 * GATHER_LAG, share_phase, early)
        at_chunk(i - LAG * STEPS - 3 * GATHER_LAG, out_phase, early)
        at_chunk(i - LAG * STEPS - 3 * GATHER_LAG - 1, lambda j: put_out(j).wait(), early)

    acc[...] = jnp.zeros_like(acc)
    ssq[...] = jnp.zeros_like(ssq)
    if COMM:
        pl.semaphore_wait(barrier, dp - 1)

    def run_layer(layer, first):
        @pl.loop(0, per // 2)
        def _(pair):
            for n in range(2):
                c = 2 * pair + n
                compute(layer, c, first + c, n == 1)
                if COMM:
                    phases(first + c)

    run_layer(1, 0)

    @pl.loop(0, tokens // FTILE)
    def _(t):
        at_t = pl.ds(pl.multiple_of(t * FTILE, FTILE), FTILE)
        wide = hv[at_t, :].astype(F32)
        scale = norm_scale(wide)
        by_a = acc[at_t, :].astype(BF16).astype(F32)
        by_h = by_a * scale - wide * (scale * scale * scale * jnp.mean(by_a * wide, -1, keepdims=True))
        by_h = dyv[at_t, :] + by_h.astype(BF16)
        dyv[at_t, :] = by_h
        wide = xv[at_t, :].astype(F32)
        a = (wide * norm_scale(wide)).astype(BF16)
        av[at_t, :] = a
        at[:, at_t] = a.T

    run_layer(0, per)

    if COMM:
        def to_peer(k):
            peer = (me + k) % dp
            return remote(ssq, ssq_all.at[me], ssq_send.at[k - 1], ssq_recv.at[k - 1], (rep, peer))

        def from_peer(k):
            peer = (me + dp - k) % dp
            return remote(ssq, ssq_all.at[peer], ssq_send.at[k - 1], ssq_recv.at[k - 1], (rep, peer))

        @pl.loop(total, total + LAG * STEPS)
        def _(i):
            phases(i)

        for k in range(1, dp):
            to_peer(k).start()
        ssq_all[me] = ssq[...]
        put_mine().start()
        for i in range(total + LAG * STEPS, early + LAG * STEPS + 3 * GATHER_LAG + 1):
            phases(i)
        for k in range(1, dp):
            to_peer(k).wait_send()
            from_peer(k).wait_recv()
        ssq_out[...] = ssq_all[...]
        put_mine().wait()
    else:
        ssq_out[...] = jnp.zeros_like(ssq_out)


def gradients(x, dy, wg, wu, wd, dp):
    tokens, d = x.shape
    layers, _, ff = wg.shape
    per = ff // CHUNK
    total = layers * per
    rows = 3 * d * ff // (per * CHUNK)
    half = rows // CORES
    chips = dp // CORES
    dma = pltpu.SemaphoreType.DMA
    return pl.pallas_call(
        functools.partial(grad_kernel, dp, layers),
        out_shape=(
            jax.ShapeDtypeStruct((total - LATE, rows, CHUNK), BF16),
            jax.ShapeDtypeStruct((LATE, rows // dp, CHUNK), BF16),
            jax.ShapeDtypeStruct((dp, 8, 128), F32),
        ),
        in_specs=[pl.BlockSpec(memory_space=pl.ANY)] * 5,
        out_specs=(pl.BlockSpec(memory_space=pl.ANY), pl.BlockSpec(memory_space=pl.ANY), pl.BlockSpec(memory_space=pltpu.VMEM)),
        scratch_shapes=[
            pltpu.VMEM((tokens, d), BF16),
            pltpu.VMEM((tokens, d), BF16),
            pltpu.VMEM((tokens, d), BF16),
            pltpu.VMEM((tokens, d), BF16),
            pltpu.VMEM((d, tokens), BF16),
            pltpu.VMEM((tokens, d), F32),
            pltpu.VMEM((FTILE, ff), BF16),
            pltpu.VMEM((tokens, CHUNK), BF16),
            pltpu.VMEM((tokens, CHUNK), BF16),
            pltpu.VMEM((tokens, 2 * CHUNK), BF16),
            pltpu.VMEM((layers, per, d, 2 * CHUNK), BF16),
            pltpu.VMEM((layers, ff, d), BF16),
            pltpu.VMEM((TERMS, rows, CHUNK), BF16),
            pltpu.VMEM((HALVES, half, CHUNK), BF16),
            pltpu.VMEM((RUNS, 4, half // chips // 2, CHUNK), BF16),
            pltpu.VMEM((RUNS, 6, half // chips // 2, CHUNK), BF16),
            pltpu.VMEM((total - LATE, rows, CHUNK), BF16),
            pltpu.VMEM((LATE, rows // dp, CHUNK), BF16),
            pltpu.VMEM((8, 128), F32),
            pltpu.VMEM((dp, 8, 128), F32),
            dma((2,)),
            dma((layers, per, 3)),
            dma((SLOTS,)),
            dma,
            dma((2, SLOTS)),
            dma((6, SLOTS)),
            dma((6, SLOTS)),
            dma((2, total)),
            dma((2, total)),
            dma((2, total)),
            dma((2, total)),
            dma((2, total)),
            dma((dp - 1,)),
            dma((dp - 1,)),
        ],
        compiler_params=pltpu.CompilerParams(collective_id=0, has_side_effects=True, vmem_limit_bytes=67043328),
        name="gradients",
    )(x, dy, wg, wu, wd)


def adamw_kernel(count, n_g, n_old, ids, ssq, *refs):
    gs, ins, outs = refs[:n_g], refs[n_g : n_g + 9], refs[n_g + 9 + n_old :]
    mean = jnp.sum(jnp.sum(ssq[...], 0), keepdims=True) / count
    factor = jnp.minimum(1.0, 0.5 * lax.rsqrt(mean + 1e-30))

    def grad(chunk, rows):
        if n_g == 1:
            return gs[0][0, chunk, rows, :].astype(F32) * factor
        value = gs[0][chunk, rows, :]
        for k in range(1, n_g):
            value = jnp.where(pl.program_id(0) == k, gs[k][chunk, rows, :], value)
        return value.astype(F32) * factor

    def one(n, index, grad):
        w, m, v = (ins[n + 3 * k] for k in range(3))
        new_w, new_m, new_v = (outs[n + 3 * k] for k in range(3))
        wide = w[index].astype(F32)
        m1 = 0.9 * m[index] + 0.1 * grad
        v1 = 0.95 * v[index] + 0.05 * grad * grad
        new_m[index] = m1
        new_v[index] = v1
        new_w[index] = (wide - 0.02 * (m1 * lax.rsqrt(v1 + 1e-8) + 0.1 * wide)).astype(BF16)

    wide_rows, d = ins[0].shape[1] // 2, ins[2].shape[4]
    tall_rows = ins[2].shape[3] // 2
    for chunk in range(PART):
        for direction in range(2):
            start = direction * (2 * wide_rows + d // CHUNK * tall_rows)
            there = (0, slice(direction * wide_rows, (direction + 1) * wide_rows), slice(chunk * CHUNK, (chunk + 1) * CHUNK))
            one(0, there, grad(chunk, slice(start, start + wide_rows)))
            one(1, there, grad(chunk, slice(start + wide_rows, start + 2 * wide_rows)))
            for k in range(d // CHUNK):
                low = start + 2 * wide_rows + k * tall_rows
                there = (0, 0, chunk, slice(direction * tall_rows, (direction + 1) * tall_rows), slice(k * CHUNK, (k + 1) * CHUNK))
                one(2, there, grad(chunk, slice(low, low + tall_rows)))


def adamw(dp, count, ids, ssq, gs, arrays, part, order, first, places, old=None):
    layers, d, ff = arrays[0].shape
    per = ff // CHUNK // PART

    def layer(p):
        return layers - 1 - p // per

    if len(gs) == 1:

        def place(i, ids):
            return part, first + i

        g_specs = [pl.BlockSpec((1, PART, gs[0].shape[2] // dp, CHUNK), lambda i, ids: (part, 0, first + i, 0))]
    else:

        def place(i, ids):
            return part, ids[first + i]

        g_specs = [pl.BlockSpec(g.shape, lambda i, ids: (0, 0, 0)) for g in gs]

    def wide_index(i, ids):
        p, s = place(i, ids)
        return layer(p), s, p % per

    def tall_index(i, ids):
        p, s = place(i, ids)
        return layer(p), p % per, 0, s, 0

    wide = pl.BlockSpec((1, d // dp, PART * CHUNK), wide_index)
    tall = pl.BlockSpec((1, 1, PART, CHUNK // dp, d), tall_index)
    trio = [wide, wide, tall]
    old = old or ()
    first_old = 2 + len(gs) + 9
    elements = places * PART * 3 * d * CHUNK // dp
    return pl.pallas_call(
        functools.partial(adamw_kernel, count, len(gs), len(old)),
        out_shape=tuple(jax.ShapeDtypeStruct(a.shape, a.dtype) for a in arrays),
        grid_spec=pltpu.PrefetchScalarGridSpec(
            num_scalar_prefetch=1,
            grid=(places,),
            in_specs=[
                pl.BlockSpec(ssq.shape, lambda i, ids: (0, 0, 0)),
                *g_specs, *trio, *trio, *trio,
                *[pl.BlockSpec(memory_space=pl.ANY)] * len(old),
            ],
            out_specs=tuple(trio * 3),
        ),
        input_output_aliases={first_old + n: n for n in range(len(old))},
        compiler_params=pltpu.CompilerParams(vmem_limit_bytes=60 * 2**20),
        cost_estimate=pl.CostEstimate(flops=elements * 40, bytes_accessed=elements * 22, transcendentals=elements),
        name=f"adamw{order}",
    )(ids, ssq, *gs, *arrays, *old)


def solution(mesh):
    dp = mesh.shape["dp"]
    chips = dp // CORES

    def step(x, dy, *arrays):
        weights = arrays[:3]
        layers, d, ff = weights[0].shape
        count = sum(w.size for w in weights)
        me = lax.axis_index("dp")
        chip, core = me // CORES, me % CORES
        turn = 1 - 2 * core
        behind, ahead, far = ((chip + chips + n) % chips for n in (-turn, turn, chips // 2))
        ids = jnp.stack([k * chips + c for k, c in (
            (core, chip), (1 - core, chip), (core, behind), (core, ahead),
            (1 - core, ahead), (1 - core, behind), (core, far), (1 - core, far),
        )])

        def index(chip, core):
            return chip % chips * CORES + core

        devices = [(c, k) for c in range(chips) for k in range(CORES)]
        on = [(index(c, k), index(c + 1 - 2 * k, k)) for c, k in devices]
        back = [(b, a) for a, b in on]
        over = [(index(c, k), index(c, 1 - k)) for c, k in devices]
        on_over = [(index(c, k), index(c + 1 - 2 * k, 1 - k)) for c, k in devices]

        g, mine, ssq = gradients(x[0], dy[0], *weights, dp)
        arrays = [a.reshape(layers, -1, PART, CHUNK, d) if n % 3 == 2 else a for n, a in enumerate(arrays)]
        g = g.reshape(-1, PART, *g.shape[1:])
        update = functools.partial(adamw, dp, count, ids, ssq)
        mine_over = lax.ppermute(mine, "dp", over)
        one = lax.ppermute(mine, "dp", on)
        two = lax.ppermute(mine, "dp", back)
        new = update([g], arrays, 0, 0, 0, FIRST)
        one, two, mine_over, new = lax.optimization_barrier((one, two, mine_over, new))
        one_over = lax.ppermute(one, "dp", over)
        two_over = lax.ppermute(two, "dp", over)
        far = lax.ppermute(one, "dp", on)
        far_over = lax.ppermute(one, "dp", on_over)
        new = update([g], arrays, 0, 1, FIRST, dp - FIRST, new)
        one_over, two_over, new = lax.optimization_barrier((one_over, two_over, new))
        near = [mine, mine_over, one, two, one_over, two_over]
        new = update(near, arrays, 1, 2, 0, len(near), new)
        far, far_over, new = lax.optimization_barrier((far, far_over, new))
        new = update([far, far_over], arrays, 1, 3, len(near), 2, new)
        return tuple(a.reshape(layers, ff, d) if n % 3 == 2 else a for n, a in enumerate(new))

    return jax.shard_map(
        step,
        mesh=mesh,
        in_specs=(P(("rep", "dp"), None, None),) * 2 + (P(None, None, None),) * 9,
        out_specs=(P("rep", None, None),) * 9,
        check_vma=False,
    )
```

```python
import functools

import jax
import jax.numpy as jnp
from jax import lax
from jax.experimental import pallas as pl
from jax.experimental.pallas import tpu as pltpu
from jax.sharding import PartitionSpec as P

MESH = pl.DeviceIdType.MESH
BF16, F32 = jnp.bfloat16, jnp.float32
CORES = 2
CHUNK = 256
TILE = 1024
FTILE = 256
LAG = 1
GATHER_LAG = 2
STEPS = 3
SLOTS = STEPS * LAG + 2
TERMS = STEPS * LAG + 1
HALVES = (STEPS + 1) * LAG + 2
RUNS = STEPS * LAG + 2
PART = 8
COMM = True


def dot(a, b):
    return jnp.dot(a, b, preferred_element_type=F32)


def dot_t(a, b):
    return lax.dot_general(a, b, (((1,), (1,)), ((), ())), preferred_element_type=F32)


def t_dot(a, b):
    return lax.dot_general(a, b, (((0,), (0,)), ((), ())), preferred_element_type=F32)


def sigmoid(z):
    return 0.5 * jnp.tanh(0.5 * z) + 0.5


def norm_scale(wide):
    return lax.rsqrt(jnp.mean(wide * wide, -1, keepdims=True) + 1e-6)


def grad_kernel(
    dp, layers, x_hbm, dy_hbm, wg_hbm, wu_hbm, wd_hbm, g_hbm, behind_hbm, ssq_out,
    xv, dyv, hv, av, acc, actf, act, by_next, dgu, wgu, wd, term, from_core, leaving, coming, g, ssq, ssq_all,
    io_sem, w_sem, out_sem, behind_sem, core_sem, ring_send, ring_recv, near_send, near_recv, share_send, share_recv, ssq_send, ssq_recv,
):
    tokens, d = xv.shape
    ff = wd_hbm.shape[1]
    per = ff // CHUNK
    total = layers * per
    chips = dp // CORES
    rows = g.shape[1]
    half = rows // CORES
    own = half // chips
    piece = own // 2
    rep = lax.axis_index("rep")
    me = lax.axis_index("dp")
    chip, core = me // CORES, me % CORES
    other = 1 - core

    def device(chip, core):
        return (rep, chip * CORES + core)

    right, left = device((chip + 1) % chips, core), device((chip + chips - 1) % chips, core)
    sibling = device(chip, other)

    barrier = pltpu.get_barrier_semaphore()
    if COMM:
        for k in range(1, dp):
            pl.semaphore_signal(barrier, inc=1, device_id=(rep, (me + k) % dp), device_id_type=MESH)

    def load_x():
        return pltpu.make_async_copy(x_hbm, xv, io_sem.at[0])

    def load_dy():
        return pltpu.make_async_copy(dy_hbm, dyv, io_sem.at[1])

    def load_w(layer):
        copies = []
        for c in range(per):
            cut = slice(c * CHUNK, (c + 1) * CHUNK)
            copies.append(pltpu.make_async_copy(wg_hbm.at[layer, :, cut], wgu.at[layer, c, :, :CHUNK], w_sem.at[layer, c, 0]))
            copies.append(pltpu.make_async_copy(wu_hbm.at[layer, :, cut], wgu.at[layer, c, :, CHUNK:], w_sem.at[layer, c, 1]))
            copies.append(pltpu.make_async_copy(wd_hbm.at[layer, cut, :], wd.at[layer, cut, :], w_sem.at[layer, c, 2]))
        return copies

    load_x().start()
    for copy in load_w(0):
        copy.start()
    load_dy().start()
    for copy in load_w(1):
        copy.start()

    load_x().wait()
    first_w = load_w(0)

    def forward(at_t, arriving):
        wide = xv[at_t, :].astype(F32)
        a = (wide * norm_scale(wide)).astype(BF16)
        for c in range(per):
            if arriving:
                for copy in first_w[3 * c : 3 * c + 3]:
                    copy.wait()
            gu = dot(a, wgu[0, c])
            gate, up = gu[:, :CHUNK], gu[:, CHUNK:]
            actf[:, c * CHUNK : (c + 1) * CHUNK] = (gate * sigmoid(gate) * up).astype(BF16)
        h = xv[at_t, :] + dot(actf[...], wd[0]).astype(BF16)
        hv[at_t, :] = h
        wide = h.astype(F32)
        av[at_t, :] = (wide * norm_scale(wide)).astype(BF16)
        acc[at_t, :] = jnp.zeros((FTILE, d), F32)

    forward(slice(0, FTILE), True)

    @pl.loop(1, tokens // FTILE)
    def _(t):
        forward(pl.ds(pl.multiple_of(t * FTILE, FTILE), FTILE), False)

    load_dy().wait()
    for copy in load_w(1):
        copy.wait()

    def compute(layer, c, i, second):
        w_chunk = wgu[layer, c]
        for t in range(tokens // TILE):
            at_t = slice(t * TILE, (t + 1) * TILE)
            gu = dot(av[at_t, :], w_chunk)
            if second:
                by_act = by_next[at_t, :].astype(F32)
            else:
                both = dot_t(dyv[at_t, :], wd[layer, pl.ds(pl.multiple_of(c * CHUNK, 2 * CHUNK), 2 * CHUNK), :]).astype(BF16)
                by_act = both[:, :CHUNK].astype(F32)
                by_next[at_t, :] = both[:, CHUNK:]
            gate, up = gu[:, :CHUNK], gu[:, CHUNK:]
            s = sigmoid(gate)
            silu = gate * s
            act[at_t, :] = (silu * up).astype(BF16)
            dgu[at_t, :CHUNK] = (by_act * up * (s + silu * (1.0 - s))).astype(BF16)
            dgu[at_t, CHUNK:] = (by_act * silu).astype(BF16)
            if layer > 0:
                by_a = dot_t(dgu[at_t, :], w_chunk)
                acc[at_t, :] += by_a
        slot = i % TERMS
        by_gu = t_dot(av[...], dgu[...]).astype(BF16)
        by_d = t_dot(act[...], dyv[...]).astype(BF16)
        blocks = rows // piece
        n, m = d // blocks, CHUNK // blocks
        for b in range(blocks):
            start = b * piece
            term[slot, start : start + n, :] = by_gu[b * n : (b + 1) * n, :CHUNK]
            term[slot, start + n : start + 2 * n, :] = by_gu[b * n : (b + 1) * n, CHUNK:]
            for k in range(d // CHUNK):
                low = start + 2 * n + k * m
                term[slot, low : low + m, :] = by_d[b * m : (b + 1) * m, k * CHUNK : (k + 1) * CHUNK]

    def remote(src, dst, send, recv, to):
        return pltpu.make_async_remote_copy(src_ref=src, dst_ref=dst, send_sem=send, recv_sem=recv, device_id=to, device_id_type=MESH)

    def rows_at(core, chip, direction=0, count=None):
        start = core * half + chip * own + direction * piece
        return pl.ds(pl.multiple_of(start, piece), piece if count is None else count)

    def swap(j):
        there = pl.ds(pl.multiple_of(other * half, half), half)
        return remote(term.at[j % TERMS, there], from_core.at[j % HALVES], core_sem.at[0, j % SLOTS], core_sem.at[1, j % SLOTS], sibling)

    def travel(j, k):
        src = leaving.at[j % RUNS, k] if k < 4 else coming.at[j % RUNS, k - 4]
        return remote(src, coming.at[j % RUNS, k], ring_send.at[k, j % SLOTS], ring_recv.at[k, j % SLOTS], right if k % 2 == 0 else left)

    def near(j, direction, arriving=False):
        if arriving:
            block = (chip + chips - 1) % chips if direction == 0 else (chip + 1) % chips
        else:
            block = chip
        place = g.at[j, rows_at(core, block, 0, own)]
        return remote(place, place, near_send.at[direction, j], near_recv.at[direction, j], right if direction == 0 else left)

    sides = (0, 1, chips - 1)

    def share(j, n, arriving=False):
        place = g.at[j, rows_at(other if arriving else core, (chip + sides[n]) % chips, 0, own)]
        return remote(place, place, share_send.at[n, j], share_recv.at[n, j], sibling)

    def put_out(j):
        copies = []
        for n in range(2 * len(sides)):
            rows_n = rows_at(n % 2, (chip + sides[n // 2]) % chips, 0, own)
            copies.append(pltpu.make_async_copy(g.at[j, rows_n], g_hbm.at[j, rows_n], out_sem.at[n, j % SLOTS]))
        return copies

    def put_behind(j):
        behind = (chip + chips - 1 + 2 * core) % chips
        return pltpu.make_async_copy(g.at[j, rows_at(core, behind, 0, own)], behind_hbm.at[j], behind_sem.at[j % SLOTS])

    def add_up(j, turn, direction, arrived=()):
        block = (chip + turn) % chips
        here = rows_at(core, block, direction)
        within = pl.ds(pl.multiple_of(block * own + direction * piece, piece), piece)
        value = term[j % TERMS, here, :].astype(F32) + from_core[j % HALVES, within, :].astype(F32)
        for k in arrived:
            value = value + coming[j % RUNS, k].astype(F32)
        return value.astype(BF16)

    def phases(i):
        def at_chunk(j, body, end=total):
            pl.when((j >= 0) & (j < end))(functools.partial(body, j))

        def start_swap(j):
            swap(j).start()

        def through(j):
            swap(j).wait()
            for k in range(2):
                leaving[j % RUNS, k] = add_up(j, chips // 2, k)
                travel(j, k).start()

        def onward(j):
            for k in range(2):
                travel(j, k).wait()
                coming[j % RUNS, k] = add_up(j, 1 if k == 0 else chips - 1, k, (k,))
                travel(j, k + 4).start()

        def alone(j):
            for k in range(2, 4):
                leaving[j % RUNS, k] = add_up(j, 1 if k == 2 else chips - 1, 3 - k)
                travel(j, k).start()

        def finish(j):
            for k in range(2, 6):
                travel(j, k).wait()
            for direction in range(2):
                value = add_up(j, 0, direction, (3 - direction, 4 + direction))
                wide = value.astype(F32)
                wide = jnp.sum((wide * wide).reshape(piece // 8, 8, CHUNK), 0)
                ssq[...] += sum(wide[:, n : n + 128] for n in range(0, CHUNK, 128))

                g[j, rows_at(core, chip, direction), :] = value
            near(j, 0).start()
            near(j, 1).start()
            share(j, 0).start()

        def spread(j):
            for direction in range(2):
                near(j, direction).wait_send()
                near(j, direction, True).wait_recv()
            for n in range(1, 3):
                share(j, n).start()
            put_behind(j).start()

        def leave(j):
            for n in range(3):
                share(j, n).wait_send()
                share(j, n, True).wait_recv()
            for copy in put_out(j):
                copy.start()

        def left_already(j):
            put_behind(j).wait()
            for copy in put_out(j):
                copy.wait()

        at_chunk(i, start_swap)
        at_chunk(i - LAG, through)
        at_chunk(i - 2 * LAG, onward)
        at_chunk(i - LAG, alone)
        at_chunk(i - 3 * LAG, finish)
        at_chunk(i - STEPS * LAG - GATHER_LAG, spread)
        at_chunk(i - STEPS * LAG - 2 * GATHER_LAG, leave)
        at_chunk(i - STEPS * LAG - 2 * GATHER_LAG - 1, left_already)

    ssq[...] = jnp.zeros_like(ssq)
    if COMM:
        pl.semaphore_wait(barrier, dp - 1)

    def run_layer(layer, first):
        @pl.loop(0, per // 2)
        def _(pair):
            for n in range(2):
                c = 2 * pair + n
                compute(layer, c, first + c, n == 1)
                if COMM:
                    phases(first + c)

    run_layer(1, 0)

    @pl.loop(0, tokens // FTILE)
    def _(t):
        at_t = pl.ds(pl.multiple_of(t * FTILE, FTILE), FTILE)
        wide = hv[at_t, :].astype(F32)
        scale = norm_scale(wide)
        by_a = acc[at_t, :].astype(BF16).astype(F32)
        by_h = by_a * scale - wide * (scale * scale * scale * jnp.mean(by_a * wide, -1, keepdims=True))
        by_h = dyv[at_t, :] + by_h.astype(BF16)
        dyv[at_t, :] = by_h
        wide = xv[at_t, :].astype(F32)
        av[at_t, :] = (wide * norm_scale(wide)).astype(BF16)

    run_layer(0, per)

    if COMM:
        def to_peer(k):
            peer = (me + k) % dp
            return remote(ssq, ssq_all.at[me], ssq_send.at[k - 1], ssq_recv.at[k - 1], (rep, peer))

        def from_peer(k):
            peer = (me + dp - k) % dp
            return remote(ssq, ssq_all.at[peer], ssq_send.at[k - 1], ssq_recv.at[k - 1], (rep, peer))

        @pl.loop(total, total + LAG * STEPS)
        def _(i):
            phases(i)

        for k in range(1, dp):
            to_peer(k).start()
        ssq_all[me] = ssq[...]
        @pl.loop(total + LAG * STEPS, total + LAG * STEPS + 2 * GATHER_LAG + 1)
        def _(i):
            phases(i)

        for k in range(1, dp):
            to_peer(k).wait_send()
            from_peer(k).wait_recv()
        ssq_out[...] = ssq_all[...]
    else:
        ssq_out[...] = jnp.zeros_like(ssq_out)


def gradients(x, dy, wg, wu, wd, dp):
    tokens, d = x.shape
    layers, _, ff = wg.shape
    per = ff // CHUNK
    total = layers * per
    rows = 3 * d * ff // (per * CHUNK)
    half = rows // CORES
    chips = dp // CORES
    dma = pltpu.SemaphoreType.DMA
    return pl.pallas_call(
        functools.partial(grad_kernel, dp, layers),
        out_shape=(
            jax.ShapeDtypeStruct((total, rows, CHUNK), BF16),
            jax.ShapeDtypeStruct((total, rows // dp, CHUNK), BF16),
            jax.ShapeDtypeStruct((dp, 8, 128), F32),
        ),
        in_specs=[pl.BlockSpec(memory_space=pl.ANY)] * 5,
        out_specs=(pl.BlockSpec(memory_space=pl.ANY), pl.BlockSpec(memory_space=pl.ANY), pl.BlockSpec(memory_space=pltpu.VMEM)),
        scratch_shapes=[
            pltpu.VMEM((tokens, d), BF16),
            pltpu.VMEM((tokens, d), BF16),
            pltpu.VMEM((tokens, d), BF16),
            pltpu.VMEM((tokens, d), BF16),
            pltpu.VMEM((tokens, d), F32),
            pltpu.VMEM((FTILE, ff), BF16),
            pltpu.VMEM((tokens, CHUNK), BF16),
            pltpu.VMEM((tokens, CHUNK), BF16),
            pltpu.VMEM((tokens, 2 * CHUNK), BF16),
            pltpu.VMEM((layers, per, d, 2 * CHUNK), BF16),
            pltpu.VMEM((layers, ff, d), BF16),
            pltpu.VMEM((TERMS, rows, CHUNK), BF16),
            pltpu.VMEM((HALVES, half, CHUNK), BF16),
            pltpu.VMEM((RUNS, 4, half // chips // 2, CHUNK), BF16),
            pltpu.VMEM((RUNS, 6, half // chips // 2, CHUNK), BF16),
            pltpu.VMEM((total, rows, CHUNK), BF16),
            pltpu.VMEM((8, 128), F32),
            pltpu.VMEM((dp, 8, 128), F32),
            dma((2,)),
            dma((layers, per, 3)),
            dma((6, SLOTS)),
            dma((SLOTS,)),
            dma((2, SLOTS)),
            dma((6, SLOTS)),
            dma((6, SLOTS)),
            dma((2, total)),
            dma((2, total)),
            dma((3, total)),
            dma((3, total)),
            dma((dp - 1,)),
            dma((dp - 1,)),
        ],
        compiler_params=pltpu.CompilerParams(collective_id=0, has_side_effects=True, vmem_limit_bytes=67043328),
        name="gradients",
    )(x, dy, wg, wu, wd)


def adamw_kernel(count, n_g, n_old, ids, ssq, *refs):
    gs, ins, outs = refs[:n_g], refs[n_g : n_g + 9], refs[n_g + 9 + n_old :]
    mean = jnp.sum(jnp.sum(ssq[...], 0), keepdims=True) / count
    factor = jnp.minimum(1.0, 0.5 * lax.rsqrt(mean + 1e-30))

    def grad(chunk, rows):
        value = gs[0][0, chunk, rows, :]
        for k in range(1, n_g):
            value = jnp.where(pl.program_id(0) % n_g == k, gs[k][0, chunk, rows, :], value)
        return value.astype(F32) * factor

    def one(n, index, grad):
        w, m, v = (ins[n + 3 * k] for k in range(3))
        new_w, new_m, new_v = (outs[n + 3 * k] for k in range(3))
        wide = w[index].astype(F32)
        m1 = 0.9 * m[index] + 0.1 * grad
        v1 = 0.95 * v[index] + 0.05 * grad * grad
        new_m[index] = m1
        new_v[index] = v1
        new_w[index] = (wide - 0.02 * (m1 * lax.rsqrt(v1 + 1e-8) + 0.1 * wide)).astype(BF16)

    wide_rows, d = ins[0].shape[1] // 2, ins[2].shape[4]
    tall_rows = ins[2].shape[3] // 2
    for chunk in range(PART):
        for direction in range(2):
            start = direction * (2 * wide_rows + d // CHUNK * tall_rows)
            there = (0, slice(direction * wide_rows, (direction + 1) * wide_rows), slice(chunk * CHUNK, (chunk + 1) * CHUNK))
            one(0, there, grad(chunk, slice(start, start + wide_rows)))
            one(1, there, grad(chunk, slice(start + wide_rows, start + 2 * wide_rows)))
            for k in range(d // CHUNK):
                low = start + 2 * wide_rows + k * tall_rows
                there = (0, 0, chunk, slice(direction * tall_rows, (direction + 1) * tall_rows), slice(k * CHUNK, (k + 1) * CHUNK))
                one(2, there, grad(chunk, slice(low, low + tall_rows)))


def adamw(dp, count, ids, ssq, gs, arrays, order, first, places, old=None):
    layers, d, ff = arrays[0].shape
    per = ff // CHUNK // PART
    parts = layers * per

    def layer(p):
        return layers - 1 - p // per

    def place(i, ids):
        return i // places, ids[first + i % places]

    if len(gs) == 1:
        g_specs = [pl.BlockSpec((1, PART, gs[0].shape[2] // dp, CHUNK), lambda i, ids: (i // places, 0, ids[first + i % places], 0))]
    else:
        g_specs = [pl.BlockSpec((1, *g.shape[1:]), lambda i, ids: (i // places, 0, 0, 0)) for g in gs]

    def wide_index(i, ids):
        p, s = place(i, ids)
        return layer(p), s, p % per

    def tall_index(i, ids):
        p, s = place(i, ids)
        return layer(p), p % per, 0, s, 0

    wide = pl.BlockSpec((1, d // dp, PART * CHUNK), wide_index)
    tall = pl.BlockSpec((1, 1, PART, CHUNK // dp, d), tall_index)
    trio = [wide, wide, tall]
    old = old or ()
    first_old = 2 + len(gs) + 9
    elements = parts * places * PART * 3 * d * CHUNK // dp
    return pl.pallas_call(
        functools.partial(adamw_kernel, count, len(gs), len(old)),
        out_shape=tuple(jax.ShapeDtypeStruct(a.shape, a.dtype) for a in arrays),
        grid_spec=pltpu.PrefetchScalarGridSpec(
            num_scalar_prefetch=1,
            grid=(parts * places,),
            in_specs=[
                pl.BlockSpec(ssq.shape, lambda i, ids: (0, 0, 0)),
                *g_specs, *trio, *trio, *trio,
                *[pl.BlockSpec(memory_space=pl.ANY)] * len(old),
            ],
            out_specs=tuple(trio * 3),
        ),
        input_output_aliases={first_old + n: n for n in range(len(old))},
        compiler_params=pltpu.CompilerParams(vmem_limit_bytes=67043328),
        cost_estimate=pl.CostEstimate(flops=elements * 40, bytes_accessed=elements * 22, transcendentals=elements),
        name=f"adamw{order}",
    )(ids, ssq, *gs, *arrays, *old)


def solution(mesh):
    dp = mesh.shape["dp"]
    chips = dp // CORES

    def step(x, dy, *arrays):
        weights = arrays[:3]
        layers, d, ff = weights[0].shape
        count = sum(w.size for w in weights)
        me = lax.axis_index("dp")
        chip, core = me // CORES, me % CORES
        turn = 1 - 2 * core
        behind, ahead, far = ((chip + chips + n) % chips for n in (-turn, turn, chips // 2))
        ids = jnp.stack([k * chips + c for k, c in (
            (core, chip), (1 - core, chip), (core, behind), (core, ahead),
            (1 - core, ahead), (1 - core, behind), (core, far), (1 - core, far),
        )])

        def index(chip, core):
            return chip % chips * CORES + core

        devices = [(c, k) for c in range(chips) for k in range(CORES)]
        on = [(index(c, k), index(c + 1 - 2 * k, k)) for c, k in devices]
        on_over = [(index(c, k), index(c + 1 - 2 * k, 1 - k)) for c, k in devices]

        g, by_behind, ssq = gradients(x[0], dy[0], *weights, dp)
        arrays = [a.reshape(layers, -1, PART, CHUNK, d) if n % 3 == 2 else a for n, a in enumerate(arrays)]
        g, by_behind = (a.reshape(-1, PART, *a.shape[1:]) for a in (g, by_behind))
        by_far = lax.ppermute(by_behind, "dp", on)
        by_far_over = lax.ppermute(by_behind, "dp", on_over)
        new = adamw(dp, count, ids, ssq, [g], arrays, 0, 0, dp - 2)
        by_far, by_far_over, new = lax.optimization_barrier((by_far, by_far_over, new))
        new = adamw(dp, count, ids, ssq, [by_far, by_far_over], arrays, 1, dp - 2, 2, new)
        return tuple(a.reshape(layers, ff, d) if n % 3 == 2 else a for n, a in enumerate(new))

    return jax.shard_map(
        step,
        mesh=mesh,
        in_specs=(P(("rep", "dp"), None, None),) * 2 + (P(None, None, None),) * 9,
        out_specs=(P("rep", None, None),) * 9,
        check_vma=False,
    )
```

```python
import functools

import jax
import jax.numpy as jnp
from jax import lax
from jax.experimental import pallas as pl
from jax.experimental.pallas import tpu as pltpu
from jax.sharding import PartitionSpec as P

MESH = pl.DeviceIdType.MESH
BF16, F32 = jnp.bfloat16, jnp.float32
CORES = 2
CHUNK = 256
TILE = 1024
FTILE = 256
LAG = 1
GATHER_LAG = 2
STEPS = 3
SLOTS = STEPS * LAG + 2
TERMS = STEPS * LAG + 1
HALVES = (STEPS + 1) * LAG + 2
RUNS = STEPS * LAG + 2
PART = 8
COMM = True


def dot(a, b):
    return jnp.dot(a, b, preferred_element_type=F32)


def dot_t(a, b):
    return lax.dot_general(a, b, (((1,), (1,)), ((), ())), preferred_element_type=F32)


def t_dot(a, b):
    return lax.dot_general(a, b, (((0,), (0,)), ((), ())), preferred_element_type=F32)


def sigmoid(z):
    return 0.5 * jnp.tanh(0.5 * z) + 0.5


def norm_scale(wide):
    return lax.rsqrt(jnp.mean(wide * wide, -1, keepdims=True) + 1e-6)


def grad_kernel(
    dp, layers, x_hbm, dy_hbm, wg_hbm, wu_hbm, wd_hbm, g_hbm, behind_hbm, ssq_out,
    xv, dyv, hv, av, acc, actf, act, by_next, dgu, wgu, wd, term, from_core, leaving, coming, g, ssq, ssq_all,
    io_sem, w_sem, out_sem, behind_sem, core_sem, ring_send, ring_recv, near_send, near_recv, share_send, share_recv, ssq_send, ssq_recv,
):
    tokens, d = xv.shape
    ff = wd_hbm.shape[1]
    per = ff // CHUNK
    total = layers * per
    chips = dp // CORES
    rows = g.shape[1]
    half = rows // CORES
    own = half // chips
    piece = own // 2
    rep = lax.axis_index("rep")
    me = lax.axis_index("dp")
    chip, core = me // CORES, me % CORES
    other = 1 - core

    def device(chip, core):
        return (rep, chip * CORES + core)

    right, left = device((chip + 1) % chips, core), device((chip + chips - 1) % chips, core)
    sibling = device(chip, other)

    barrier = pltpu.get_barrier_semaphore()
    if COMM:
        for k in range(1, dp):
            pl.semaphore_signal(barrier, inc=1, device_id=(rep, (me + k) % dp), device_id_type=MESH)

    def load_x():
        return pltpu.make_async_copy(x_hbm, xv, io_sem.at[0])

    def load_dy():
        return pltpu.make_async_copy(dy_hbm, dyv, io_sem.at[1])

    def load_w(layer):
        copies = []
        for c in range(per):
            cut = slice(c * CHUNK, (c + 1) * CHUNK)
            copies.append(pltpu.make_async_copy(wg_hbm.at[layer, :, cut], wgu.at[layer, c, :, :CHUNK], w_sem.at[layer, c, 0]))
            copies.append(pltpu.make_async_copy(wu_hbm.at[layer, :, cut], wgu.at[layer, c, :, CHUNK:], w_sem.at[layer, c, 1]))
            copies.append(pltpu.make_async_copy(wd_hbm.at[layer, cut, :], wd.at[layer, cut, :], w_sem.at[layer, c, 2]))
        return copies

    load_x().start()
    for copy in load_w(0):
        copy.start()
    load_dy().start()
    for copy in load_w(1):
        copy.start()

    load_x().wait()
    first_w = load_w(0)

    def forward(at_t, arriving):
        wide = xv[at_t, :].astype(F32)
        a = (wide * norm_scale(wide)).astype(BF16)
        for c in range(per):
            if arriving:
                for copy in first_w[3 * c : 3 * c + 3]:
                    copy.wait()
            gu = dot(a, wgu[0, c])
            gate, up = gu[:, :CHUNK], gu[:, CHUNK:]
            actf[:, c * CHUNK : (c + 1) * CHUNK] = (gate * sigmoid(gate) * up).astype(BF16)
        h = xv[at_t, :] + dot(actf[...], wd[0]).astype(BF16)
        hv[at_t, :] = h
        wide = h.astype(F32)
        av[at_t, :] = (wide * norm_scale(wide)).astype(BF16)
        acc[at_t, :] = jnp.zeros((FTILE, d), F32)

    forward(slice(0, FTILE), True)

    @pl.loop(1, tokens // FTILE)
    def _(t):
        forward(pl.ds(pl.multiple_of(t * FTILE, FTILE), FTILE), False)

    load_dy().wait()
    for copy in load_w(1):
        copy.wait()

    def compute(layer, c, i, second, between):
        w_chunk = wgu[layer, c]
        for t in range(tokens // TILE):
            at_t = slice(t * TILE, (t + 1) * TILE)
            gu = dot(av[at_t, :], w_chunk)
            if second:
                by_act = by_next[at_t, :].astype(F32)
            else:
                both = dot_t(dyv[at_t, :], wd[layer, pl.ds(pl.multiple_of(c * CHUNK, 2 * CHUNK), 2 * CHUNK), :]).astype(BF16)
                by_act = both[:, :CHUNK].astype(F32)
                by_next[at_t, :] = both[:, CHUNK:]
            gate, up = gu[:, :CHUNK], gu[:, CHUNK:]
            s = sigmoid(gate)
            silu = gate * s
            act[at_t, :] = (silu * up).astype(BF16)
            dgu[at_t, :CHUNK] = (by_act * up * (s + silu * (1.0 - s))).astype(BF16)
            dgu[at_t, CHUNK:] = (by_act * silu).astype(BF16)
            if layer > 0:
                by_a = dot_t(dgu[at_t, :], w_chunk)
                acc[at_t, :] += by_a
            if t == 0:
                between()
        slot = i % TERMS
        by_gu = t_dot(av[...], dgu[...]).astype(BF16)
        by_d = t_dot(act[...], dyv[...]).astype(BF16)
        blocks = rows // piece
        n, m = d // blocks, CHUNK // blocks
        for b in range(blocks):
            start = b * piece
            term[slot, start : start + n, :] = by_gu[b * n : (b + 1) * n, :CHUNK]
            term[slot, start + n : start + 2 * n, :] = by_gu[b * n : (b + 1) * n, CHUNK:]
            for k in range(d // CHUNK):
                low = start + 2 * n + k * m
                term[slot, low : low + m, :] = by_d[b * m : (b + 1) * m, k * CHUNK : (k + 1) * CHUNK]

    def remote(src, dst, send, recv, to):
        return pltpu.make_async_remote_copy(src_ref=src, dst_ref=dst, send_sem=send, recv_sem=recv, device_id=to, device_id_type=MESH)

    def rows_at(core, chip, direction=0, count=None):
        start = core * half + chip * own + direction * piece
        return pl.ds(pl.multiple_of(start, piece), piece if count is None else count)

    def swap(j):
        there = pl.ds(pl.multiple_of(other * half, half), half)
        return remote(term.at[j % TERMS, there], from_core.at[j % HALVES], core_sem.at[0, j % SLOTS], core_sem.at[1, j % SLOTS], sibling)

    def travel(j, k):
        src = leaving.at[j % RUNS, k] if k < 4 else coming.at[j % RUNS, k - 4]
        return remote(src, coming.at[j % RUNS, k], ring_send.at[k, j % SLOTS], ring_recv.at[k, j % SLOTS], right if k % 2 == 0 else left)

    def near(j, direction, arriving=False):
        if arriving:
            block = (chip + chips - 1) % chips if direction == 0 else (chip + 1) % chips
        else:
            block = chip
        place = g.at[j, rows_at(core, block, 0, own)]
        return remote(place, place, near_send.at[direction, j], near_recv.at[direction, j], right if direction == 0 else left)

    sides = (0, 1, chips - 1)

    def share(j, n, arriving=False):
        place = g.at[j, rows_at(other if arriving else core, (chip + sides[n]) % chips, 0, own)]
        return remote(place, place, share_send.at[n, j], share_recv.at[n, j], sibling)

    def put_out(j):
        copies = []
        for n in range(2 * len(sides)):
            rows_n = rows_at(n % 2, (chip + sides[n // 2]) % chips, 0, own)
            copies.append(pltpu.make_async_copy(g.at[j, rows_n], g_hbm.at[j, rows_n], out_sem.at[n, j % SLOTS]))
        return copies

    def put_behind(j):
        behind = (chip + chips - 1 + 2 * core) % chips
        return pltpu.make_async_copy(g.at[j, rows_at(core, behind, 0, own)], behind_hbm.at[j], behind_sem.at[j % SLOTS])

    def add_up(j, turn, direction, arrived=()):
        block = (chip + turn) % chips
        here = rows_at(core, block, direction)
        within = pl.ds(pl.multiple_of(block * own + direction * piece, piece), piece)
        value = term[j % TERMS, here, :].astype(F32) + from_core[j % HALVES, within, :].astype(F32)
        for k in arrived:
            value = value + coming[j % RUNS, k].astype(F32)
        return value.astype(BF16)

    def phases(i):
        def at_chunk(j, body, end=total):
            pl.when((j >= 0) & (j < end))(functools.partial(body, j))

        def through(j):
            swap(j).wait()
            for k in range(2):
                leaving[j % RUNS, k] = add_up(j, chips // 2, k)
                travel(j, k).start()

        def onward(j):
            for k in range(2):
                travel(j, k).wait()
                coming[j % RUNS, k] = add_up(j, 1 if k == 0 else chips - 1, k, (k,))
                travel(j, k + 4).start()

        def alone(j):
            for k in range(2, 4):
                leaving[j % RUNS, k] = add_up(j, 1 if k == 2 else chips - 1, 3 - k)
                travel(j, k).start()

        def finish(j):
            for k in range(2, 6):
                travel(j, k).wait()
            for direction in range(2):
                value = add_up(j, 0, direction, (3 - direction, 4 + direction))
                wide = value.astype(F32)
                wide = jnp.sum((wide * wide).reshape(piece // 8, 8, CHUNK), 0)
                ssq[...] += sum(wide[:, n : n + 128] for n in range(0, CHUNK, 128))

                g[j, rows_at(core, chip, direction), :] = value
            near(j, 0).start()
            near(j, 1).start()
            share(j, 0).start()

        def spread(j):
            for direction in range(2):
                near(j, direction).wait_send()
                near(j, direction, True).wait_recv()
            for n in range(1, 3):
                share(j, n).start()
            put_behind(j).start()

        def leave(j):
            for n in range(3):
                share(j, n).wait_send()
                share(j, n, True).wait_recv()
            for copy in put_out(j):
                copy.start()

        def left_already(j):
            put_behind(j).wait()
            for copy in put_out(j):
                copy.wait()

        at_chunk(i - LAG, through)
        at_chunk(i - 2 * LAG, onward)
        at_chunk(i - LAG, alone)
        at_chunk(i - 3 * LAG, finish)
        at_chunk(i - STEPS * LAG - GATHER_LAG, spread)
        at_chunk(i - STEPS * LAG - 2 * GATHER_LAG, leave)
        at_chunk(i - STEPS * LAG - 2 * GATHER_LAG - 1, left_already)

    ssq[...] = jnp.zeros_like(ssq)
    if COMM:
        pl.semaphore_wait(barrier, dp - 1)

    def run_layer(layer, first):
        @pl.loop(0, per // 2)
        def _(pair):
            for n in range(2):
                c = 2 * pair + n
                compute(layer, c, first + c, n == 1, functools.partial(phases, first + c) if COMM else lambda: None)
                if COMM:
                    swap(first + c).start()

    run_layer(1, 0)

    @pl.loop(0, tokens // FTILE)
    def _(t):
        at_t = pl.ds(pl.multiple_of(t * FTILE, FTILE), FTILE)
        wide = hv[at_t, :].astype(F32)
        scale = norm_scale(wide)
        by_a = acc[at_t, :].astype(BF16).astype(F32)
        by_h = by_a * scale - wide * (scale * scale * scale * jnp.mean(by_a * wide, -1, keepdims=True))
        by_h = dyv[at_t, :] + by_h.astype(BF16)
        dyv[at_t, :] = by_h
        wide = xv[at_t, :].astype(F32)
        av[at_t, :] = (wide * norm_scale(wide)).astype(BF16)

    run_layer(0, per)

    if COMM:
        def to_peer(k):
            peer = (me + k) % dp
            return remote(ssq, ssq_all.at[me], ssq_send.at[k - 1], ssq_recv.at[k - 1], (rep, peer))

        def from_peer(k):
            peer = (me + dp - k) % dp
            return remote(ssq, ssq_all.at[peer], ssq_send.at[k - 1], ssq_recv.at[k - 1], (rep, peer))

        @pl.loop(total, total + LAG * STEPS)
        def _(i):
            phases(i)

        for k in range(1, dp):
            to_peer(k).start()
        ssq_all[me] = ssq[...]
        @pl.loop(total + LAG * STEPS, total + LAG * STEPS + 2 * GATHER_LAG + 1)
        def _(i):
            phases(i)

        for k in range(1, dp):
            to_peer(k).wait_send()
            from_peer(k).wait_recv()
        ssq_out[...] = ssq_all[...]
    else:
        ssq_out[...] = jnp.zeros_like(ssq_out)


def gradients(x, dy, wg, wu, wd, dp):
    tokens, d = x.shape
    layers, _, ff = wg.shape
    per = ff // CHUNK
    total = layers * per
    rows = 3 * d * ff // (per * CHUNK)
    half = rows // CORES
    chips = dp // CORES
    dma = pltpu.SemaphoreType.DMA
    return pl.pallas_call(
        functools.partial(grad_kernel, dp, layers),
        out_shape=(
            jax.ShapeDtypeStruct((total, rows, CHUNK), BF16),
            jax.ShapeDtypeStruct((total, rows // dp, CHUNK), BF16),
            jax.ShapeDtypeStruct((dp, 8, 128), F32),
        ),
        in_specs=[pl.BlockSpec(memory_space=pl.ANY)] * 5,
        out_specs=(pl.BlockSpec(memory_space=pl.ANY), pl.BlockSpec(memory_space=pl.ANY), pl.BlockSpec(memory_space=pltpu.VMEM)),
        scratch_shapes=[
            pltpu.VMEM((tokens, d), BF16),
            pltpu.VMEM((tokens, d), BF16),
            pltpu.VMEM((tokens, d), BF16),
            pltpu.VMEM((tokens, d), BF16),
            pltpu.VMEM((tokens, d), F32),
            pltpu.VMEM((FTILE, ff), BF16),
            pltpu.VMEM((tokens, CHUNK), BF16),
            pltpu.VMEM((tokens, CHUNK), BF16),
            pltpu.VMEM((tokens, 2 * CHUNK), BF16),
            pltpu.VMEM((layers, per, d, 2 * CHUNK), BF16),
            pltpu.VMEM((layers, ff, d), BF16),
            pltpu.VMEM((TERMS, rows, CHUNK), BF16),
            pltpu.VMEM((HALVES, half, CHUNK), BF16),
            pltpu.VMEM((RUNS, 4, half // chips // 2, CHUNK), BF16),
            pltpu.VMEM((RUNS, 6, half // chips // 2, CHUNK), BF16),
            pltpu.VMEM((total, rows, CHUNK), BF16),
            pltpu.VMEM((8, 128), F32),
            pltpu.VMEM((dp, 8, 128), F32),
            dma((2,)),
            dma((layers, per, 3)),
            dma((6, SLOTS)),
            dma((SLOTS,)),
            dma((2, SLOTS)),
            dma((6, SLOTS)),
            dma((6, SLOTS)),
            dma((2, total)),
            dma((2, total)),
            dma((3, total)),
            dma((3, total)),
            dma((dp - 1,)),
            dma((dp - 1,)),
        ],
        compiler_params=pltpu.CompilerParams(collective_id=0, has_side_effects=True, vmem_limit_bytes=67043328),
        name="gradients",
    )(x, dy, wg, wu, wd)


def adamw_kernel(count, n_g, n_old, ids, ssq, *refs):
    gs, ins, outs = refs[:n_g], refs[n_g : n_g + 9], refs[n_g + 9 + n_old :]
    mean = jnp.sum(jnp.sum(ssq[...], 0), keepdims=True) / count
    factor = jnp.minimum(1.0, 0.5 * lax.rsqrt(mean + 1e-30))

    def grad(chunk, rows):
        value = gs[0][0, chunk, rows, :]
        for k in range(1, n_g):
            value = jnp.where(pl.program_id(0) % n_g == k, gs[k][0, chunk, rows, :], value)
        return value.astype(F32) * factor

    def one(n, index, grad):
        w, m, v = (ins[n + 3 * k] for k in range(3))
        new_w, new_m, new_v = (outs[n + 3 * k] for k in range(3))
        wide = w[index].astype(F32)
        m1 = 0.9 * m[index] + 0.1 * grad
        v1 = 0.95 * v[index] + 0.05 * grad * grad
        new_m[index] = m1
        new_v[index] = v1
        new_w[index] = (wide - 0.02 * (m1 * lax.rsqrt(v1 + 1e-8) + 0.1 * wide)).astype(BF16)

    wide_rows, d = ins[0].shape[1] // 2, ins[2].shape[4]
    tall_rows = ins[2].shape[3] // 2
    for chunk in range(PART):
        for direction in range(2):
            start = direction * (2 * wide_rows + d // CHUNK * tall_rows)
            there = (0, slice(direction * wide_rows, (direction + 1) * wide_rows), slice(chunk * CHUNK, (chunk + 1) * CHUNK))
            one(0, there, grad(chunk, slice(start, start + wide_rows)))
            one(1, there, grad(chunk, slice(start + wide_rows, start + 2 * wide_rows)))
            for k in range(d // CHUNK):
                low = start + 2 * wide_rows + k * tall_rows
                there = (0, 0, chunk, slice(direction * tall_rows, (direction + 1) * tall_rows), slice(k * CHUNK, (k + 1) * CHUNK))
                one(2, there, grad(chunk, slice(low, low + tall_rows)))


def adamw(dp, count, ids, ssq, gs, arrays, order, first, places, old=None):
    layers, d, ff = arrays[0].shape
    per = ff // CHUNK // PART
    parts = layers * per

    def layer(p):
        return layers - 1 - p // per

    def place(i, ids):
        return i // places, ids[first + i % places]

    if len(gs) == 1:
        g_specs = [pl.BlockSpec((1, PART, gs[0].shape[2] // dp, CHUNK), lambda i, ids: (i // places, 0, ids[first + i % places], 0))]
    else:
        g_specs = [pl.BlockSpec((1, *g.shape[1:]), lambda i, ids: (i // places, 0, 0, 0)) for g in gs]

    def wide_index(i, ids):
        p, s = place(i, ids)
        return layer(p), s, p % per

    def tall_index(i, ids):
        p, s = place(i, ids)
        return layer(p), p % per, 0, s, 0

    wide = pl.BlockSpec((1, d // dp, PART * CHUNK), wide_index)
    tall = pl.BlockSpec((1, 1, PART, CHUNK // dp, d), tall_index)
    trio = [wide, wide, tall]
    old = old or ()
    first_old = 2 + len(gs) + 9
    elements = parts * places * PART * 3 * d * CHUNK // dp
    return pl.pallas_call(
        functools.partial(adamw_kernel, count, len(gs), len(old)),
        out_shape=tuple(jax.ShapeDtypeStruct(a.shape, a.dtype) for a in arrays),
        grid_spec=pltpu.PrefetchScalarGridSpec(
            num_scalar_prefetch=1,
            grid=(parts * places,),
            in_specs=[
                pl.BlockSpec(ssq.shape, lambda i, ids: (0, 0, 0)),
                *g_specs, *trio, *trio, *trio,
                *[pl.BlockSpec(memory_space=pl.ANY)] * len(old),
            ],
            out_specs=tuple(trio * 3),
        ),
        input_output_aliases={first_old + n: n for n in range(len(old))},
        compiler_params=pltpu.CompilerParams(vmem_limit_bytes=67043328),
        cost_estimate=pl.CostEstimate(flops=elements * 40, bytes_accessed=elements * 22, transcendentals=elements),
        name=f"adamw{order}",
    )(ids, ssq, *gs, *arrays, *old)


def solution(mesh):
    dp = mesh.shape["dp"]
    chips = dp // CORES

    def step(x, dy, *arrays):
        weights = arrays[:3]
        layers, d, ff = weights[0].shape
        count = sum(w.size for w in weights)
        me = lax.axis_index("dp")
        chip, core = me // CORES, me % CORES
        turn = 1 - 2 * core
        behind, ahead, far = ((chip + chips + n) % chips for n in (-turn, turn, chips // 2))
        ids = jnp.stack([k * chips + c for k, c in (
            (core, chip), (1 - core, chip), (core, behind), (core, ahead),
            (1 - core, ahead), (1 - core, behind), (core, far), (1 - core, far),
        )])

        def index(chip, core):
            return chip % chips * CORES + core

        devices = [(c, k) for c in range(chips) for k in range(CORES)]
        on = [(index(c, k), index(c + 1 - 2 * k, k)) for c, k in devices]
        on_over = [(index(c, k), index(c + 1 - 2 * k, 1 - k)) for c, k in devices]

        g, by_behind, ssq = gradients(x[0], dy[0], *weights, dp)
        arrays = [a.reshape(layers, -1, PART, CHUNK, d) if n % 3 == 2 else a for n, a in enumerate(arrays)]
        g, by_behind = (a.reshape(-1, PART, *a.shape[1:]) for a in (g, by_behind))
        by_far = lax.ppermute(by_behind, "dp", on)
        by_far_over = lax.ppermute(by_behind, "dp", on_over)
        new = adamw(dp, count, ids, ssq, [g], arrays, 0, 0, dp - 2)
        by_far, by_far_over, new = lax.optimization_barrier((by_far, by_far_over, new))
        new = adamw(dp, count, ids, ssq, [by_far, by_far_over], arrays, 1, dp - 2, 2, new)
        return tuple(a.reshape(layers, ff, d) if n % 3 == 2 else a for n, a in enumerate(new))

    return jax.shard_map(
        step,
        mesh=mesh,
        in_specs=(P(("rep", "dp"), None, None),) * 2 + (P(None, None, None),) * 9,
        out_specs=(P("rep", None, None),) * 9,
        check_vma=False,
    )
```
